256 devices in a mesh: tm: 64 (over y, z, x_hi), space: 4 (over x_lo, core).
Axes of the slice: x: 4 (x_hi: 2, x_lo: 2; x = x_hi * 2 + x_lo), y: 4, z: 8, core: 2. Of those that a mesh axis runs over, the one named last changes fastest.
Arguments:
- initial: float32 [8, 128, 128], P('space'), may hold values from -6 to 6
- start_guess: float32 [64, 8, 128, 128], P('tm', 'space'), may hold values from -6 to 6
- forcing: float32 [64, 5, 8, 128, 128], P('tm', None, 'space'), may hold values from -6 to 6
- step_size: float32 [64], P('tm'), may hold values from 0.06 to 0.16
Outputs:
- fine_values: float32 [64, 5, 8, 128, 128], P('tm', None, 'space')
The draws below stay inside these ranges and needn't reach their ends.
All inputs are finite; a program needn't handle non-finite values.
Results may differ from the reference program's by a relative error of at most 0.0001.
Values sent between devices are 32-bit elements; how exact they have to be, the bound alone decides.
A program may use at most 64 MiB of HBM per device.

```python
import math
import jax
import jax.numpy as jnp
import numpy as np
from jax import lax

NX = 128
NY = 128
NODES = 5
ITERS = 2
NTIME = 64
NZ = 8


def level_of(rng, shape, cuts, low, top_value):
    gain, own = 1.0, jax.random.fold_in(rng, 6)
    for axis_at, blocks in cuts:
        steps = jnp.exp(jax.random.uniform(jax.random.fold_in(own, axis_at), (blocks,), jnp.float32, low / len(cuts), top_value / len(cuts)))
        gain = gain * jnp.repeat(steps, shape[axis_at] // blocks).reshape([-1 if axis == axis_at else 1 for axis in range(len(shape))])
    return gain


def centred(stream_key, shape, scale, bound, shards=(), kind=jnp.bfloat16):
    result = scale * jax.random.normal(stream_key, shape, jnp.float32)
    if shards:
        result = result * level_of(stream_key, shape, shards, -0.22, 0.18)
    return jnp.clip(result, -bound, bound).astype(kind)


def setup_inputs(seed: int = 0) -> dict:
    arg_keys = jax.random.split(jax.random.key(seed), 5)
    return {
        "initial": centred(arg_keys[0], (NZ, NX, NY), 1.0, 6.0, ((0, 4),), jnp.float32),
        "start_guess": centred(arg_keys[1], (NTIME, NZ, NX, NY), 1.0, 6.0, ((0, 64), (1, 4)), jnp.float32),
        "forcing": centred(arg_keys[2], (NTIME, NODES, NZ, NX, NY), 1.0, 6.0, ((0, 64), (2, 4)), jnp.float32),
        "step_size": jnp.clip(jnp.exp(math.log(0.16) - 0.98082925 * jax.random.uniform(arg_keys[3], (NTIME,), jnp.float32) ** level_of(arg_keys[3], (NTIME,), ((0, 64),), -0.2, 0.2)), 0.06, 0.16),
    }


def node_tables():
    radical = math.sqrt(3.0 / 7.0)
    node_times = [0.0, (1.0 - radical) / 2.0, 0.5, (1.0 + radical) / 2.0, 1.0]
    integrals = np.zeros((4, 5))
    for column in range(5):
        coeffs = [1.0]
        for other_index in range(5):
            if other_index == column:
                continue
            other_time = node_times[other_index]
            scaling = node_times[column] - other_time
            grown = [0.0] * (len(coeffs) + 1)
            for exponent in range(len(coeffs)):
                grown[exponent + 1] += coeffs[exponent] / scaling
                grown[exponent] -= coeffs[exponent] * other_time / scaling
            coeffs = grown
        for section in range(4):
            integrals[section, column] = sum((coeffs[exponent] * (node_times[section + 1] ** (exponent + 1) - node_times[section] ** (exponent + 1)) / (exponent + 1) for exponent in range(len(coeffs))))
    coarse = [0.0, 0.5, 1.0]
    interp = np.zeros((5, 3))
    for column in range(3):
        for section in range(5):
            weight = 1.0
            for other_index in range(3):
                if other_index != column:
                    weight = weight * (node_times[section] - coarse[other_index]) / (coarse[column] - coarse[other_index])
            interp[section, column] = weight
    return (np.array(node_times), integrals, interp)

def laplace(field):
    widths = [(0, 0)] * (field.ndim - 3) + [(1, 1)] * 3
    padded = jnp.pad(field, widths)
    center = padded[..., 1:-1, 1:-1, 1:-1]
    return padded[..., 2:, 1:-1, 1:-1] + padded[..., :-2, 1:-1, 1:-1] + padded[..., 1:-1, 2:, 1:-1] + padded[..., 1:-1, :-2, 1:-1] + padded[..., 1:-1, 1:-1, 2:] + padded[..., 1:-1, 1:-1, :-2] - 6.0 * center

def fine_sweep(values, forcing, full_step, node_times, integrals):
    half_step = 0.5 * full_step
    lap_old = laplace(values)
    rates = lap_old + forcing
    swept = [values[0]]
    lap_new = [lap_old[0]]
    for section in range(4):
        quadrature = sum((float(integrals[section, column]) * rates[column] for column in range(5)))
        spacing = float(node_times[section + 1] - node_times[section])
        advanced = swept[section] + full_step * spacing * (lap_new[section] - lap_old[section]) + full_step * quadrature
        swept.append(advanced)
        lap_new.append(laplace(advanced))
    new_rates = [lap_new[column] + forcing[column] for column in range(5)]
    first_half = full_step * sum((float(integrals[0, column] + integrals[1, column]) * new_rates[column] for column in range(5)))
    second_half = full_step * sum((float(integrals[2, column] + integrals[3, column]) * new_rates[column] for column in range(5)))
    left = first_half - half_step * lap_new[0]
    right = second_half - half_step * lap_new[2]
    return (jnp.stack(swept), left, right)

def reference(initial, start_guess, forcing, step_size):
    node_times, integrals, interp = node_tables()
    values = jnp.broadcast_to(start_guess[:, None], (NTIME, NODES, NZ, NX, NY))

    def link(start_value, packed):
        left_term, right_term, half_step = packed
        middle = start_value + half_step * laplace(start_value) + left_term
        ending = middle + half_step * laplace(middle) + right_term
        return (ending, (start_value, middle, ending))
    for sweep_round in range(ITERS):
        starts = jnp.concatenate([initial[None], values[:-1, NODES - 1]], axis=0)
        values = values.at[:, 0].set(starts)
        swept, left, right = lax.map(lambda packed: fine_sweep(packed[0], packed[1], packed[2], node_times, integrals), (values, forcing, step_size))
        last_value, coarse = lax.scan(link, initial, (left, right, 0.5 * step_size))
        deltas = [coarse[0] - swept[:, 0], coarse[1] - swept[:, 2], coarse[2] - swept[:, 4]]
        values = jnp.stack([swept[:, section] + sum((float(interp[section, column]) * deltas[column] for column in range(3))) for section in range(5)], axis=1)
    return values
```

```python
import functools
import math

import jax
import jax.numpy as jnp
import numpy as np
from jax import lax
from jax.experimental import pallas as pl
from jax.experimental.pallas import tpu as pltpu
from jax.sharding import PartitionSpec as P

MESH = pl.DeviceIdType.MESH
GROUPS = 4


def node_tables():
    radical = math.sqrt(3.0 / 7.0)
    times = [0.0, (1.0 - radical) / 2.0, 0.5, (1.0 + radical) / 2.0, 1.0]
    integrals = np.zeros((4, 5))
    for column in range(5):
        coeffs = np.array([1.0])
        for other in range(5):
            if other != column:
                coeffs = np.convolve(coeffs, [-times[other], 1.0]) / (times[column] - times[other])
        powers = np.arange(1, 6)
        for section in range(4):
            integrals[section, column] = np.sum(
                coeffs * (times[section + 1] ** powers - times[section] ** powers) / powers
            )
    coarse = [0.0, 0.5, 1.0]
    interp = np.zeros((5, 3))
    for column in range(3):
        for section in range(5):
            weight = 1.0
            for other in range(3):
                if other != column:
                    weight *= (times[section] - coarse[other]) / (coarse[column] - coarse[other])
            interp[section, column] = weight
    return times, integrals, interp


TIMES, QUAD, INTERP = node_tables()
SPACING = [TIMES[m + 1] - TIMES[m] for m in range(4)]


def mixed(weights, values):
    total = None
    for weight, value in zip(weights, values):
        if value is None or abs(weight) < 1e-14:
            continue
        term = float(weight) * value
        total = term if total is None else total + term
    return total


def sweep(u, q, mu):
    v = [u[0]]
    for m in range(4):
        weights = list(QUAD[m])
        weights[m] -= SPACING[m]
        rate = mixed(weights + [SPACING[m]], u + [v[m]])
        new = -mu * rate
        if q is not None:
            new = new + q[m]
        if v[m] is not None:
            new = new + v[m]
        v.append(new)
    return v


def coarse_terms(v, q, mu):
    weights = QUAD[0] + QUAD[1]
    weights[0] -= 0.5
    left = -mu * mixed(weights, v)
    weights = QUAD[2] + QUAD[3]
    weights[2] -= 0.5
    right = -mu * mixed(weights, v)
    if q is not None:
        left = left + (q[0] + q[1])
        right = right + (q[2] + q[3])
    return left, right


def sources(q, guess, before, mu):
    rho = 1.0 - 0.5 * mu
    v = sweep([before, guess, guess, guess, guess], q, mu)
    left, right = coarse_terms(v, q, mu)
    forced = rho * left + right
    u = [None, None, left, None, forced]
    for m in (1, 3):
        u[m] = v[m] + mixed(INTERP[m], [-before, left - v[2], forced - v[4]])
    v = sweep(u, q, mu)
    left2, right2 = coarse_terms(v, q, mu)
    return forced, v, left2, rho * left2 + right2


def responses(mu):
    rho = 1.0 - 0.5 * mu
    square = rho * rho
    u = [1.0, None, rho, None, square]
    for m in (1, 3):
        u[m] = float(INTERP[m, 0]) + float(INTERP[m, 1]) * rho + float(INTERP[m, 2]) * square
    v = sweep(u, None, mu)
    left, right = coarse_terms(v, None, mu)
    return rho, square, v, left, rho * left + right


def sine(length):
    k = np.arange(1, length + 1)
    return math.sqrt(2.0 / (length + 1)) * np.sin(math.pi / (length + 1) * np.outer(k, k))


def eigen(length):
    return 2.0 - 2.0 * np.cos(math.pi / (length + 1) * np.arange(1, length + 1))


def along_z(planes, matrix):
    n = len(planes)
    half = n // 2
    even = [planes[i] + planes[n - 1 - i] for i in range(half)]
    odd = [planes[i] - planes[n - 1 - i] for i in range(half)]
    out = []
    for k in range(n):
        out.append(mixed(matrix[k][:half], even if k % 2 == 0 else odd))
    return out


def kernel(
    sizes, start_hbm, force_hbm, first_hbm, step_ref, sin_ref, lamxy_ref, out_hbm,
    f_raw, g_raw, i_raw, b_raw, hat, recv, lam, spec, fb, keep, steps, scan_in, gains, gain_all,
    prefix, totals, cd, beta, yout, outr, res,
    load_sem, store_sem, in_send, in_recv, shift_sem, step_send, step_recv, scan_send, scan_recv,
    gain_send, gain_recv, tot_send, tot_recv, back_send, back_recv, out_send, out_recv,
):
    count, spaces, nx, ny, nz = sizes
    per = count // GROUPS
    depth = nz // spaces
    cols = nx // spaces
    rows = nz * cols
    part = rows // per
    high = lax.Precision.HIGHEST
    tm = lax.axis_index("tm")
    sp = lax.axis_index("space")
    group = tm // per
    slot = tm % per

    def dot(a, b):
        return jnp.dot(a, b, precision=high, preferred_element_type=jnp.float32)

    loads = [
        pltpu.make_async_copy(force_hbm.at[0], f_raw, load_sem.at[0]),
        pltpu.make_async_copy(start_hbm.at[0], g_raw, load_sem.at[1]),
        pltpu.make_async_copy(first_hbm, i_raw, load_sem.at[2]),
    ]
    for load in loads:
        load.start()

    barrier = pltpu.get_barrier_semaphore()

    def greet(target):
        pl.semaphore_signal(barrier, inc=1, device_id=target, device_id_type=MESH)

    following = (lax.rem(tm + 1, count), sp)
    preceding = (lax.rem(tm + count - 1, count), sp)
    for d in range(1, spaces):
        greet((tm, lax.rem(sp + d, spaces)))
    for d in range(1, per):
        greet((group * per + lax.rem(slot + d, per), sp))
    for d in range(1, GROUPS):
        greet((lax.rem(group + d, GROUPS) * per + slot, sp))
    greet(following)
    greet(preceding)

    step = step_ref[0]
    z_eigen = eigen(nz)
    here = lamxy_ref[pl.ds(pl.multiple_of(sp * cols, cols), cols), :]
    for k in range(nz):
        lam[pl.ds(k * cols, cols), :] = here + float(z_eigen[k])
    steps[slot] = jnp.full((8, ny), step, jnp.float32)

    pl.semaphore_wait(barrier, spaces + per + GROUPS - 1)

    for load in loads:
        load.wait()
    shift = pltpu.make_async_remote_copy(
        src_ref=g_raw, dst_ref=b_raw, send_sem=shift_sem.at[0], recv_sem=shift_sem.at[1],
        device_id=following, device_id_type=MESH,
    )
    shift.start()
    step_copies = []
    for d in range(1, per):
        copy = pltpu.make_async_remote_copy(
            src_ref=steps.at[slot], dst_ref=steps.at[slot],
            send_sem=step_send.at[d - 1], recv_sem=step_recv.at[d - 1],
            device_id=(group * per + lax.rem(slot + d, per), sp), device_id_type=MESH,
        )
        copy.start()
        step_copies.append(copy)

    in_copies = []

    def hand_out(f):
        mine = pl.multiple_of(sp * cols, cols)
        recv[f, pl.ds(sp * depth, depth)] = hat[f, :, pl.ds(mine, cols), :]
        for d in range(1, spaces):
            other = lax.rem(sp + d, spaces)
            copy = pltpu.make_async_remote_copy(
                src_ref=hat.at[f, :, pl.ds(pl.multiple_of(other * cols, cols), cols), :],
                dst_ref=recv.at[f, pl.ds(sp * depth, depth)],
                send_sem=in_send.at[f, d - 1], recv_sem=in_recv.at[f, d - 1],
                device_id=(tm, other), device_id_type=MESH,
            )
            copy.start()
            in_copies.append(copy)

    for m in range(4):
        for z in range(depth):
            q = step * mixed(QUAD[m], [f_raw[j, z] for j in range(5)])
            hat[m, z] = dot(dot(sin_ref[...], q), sin_ref[...])
        hand_out(m)
    for z in range(depth):
        hat[4, z] = dot(dot(sin_ref[...], g_raw[z]), sin_ref[...])
    hand_out(4)
    shift.wait_recv()
    for z in range(depth):
        before = jnp.where(tm == 0, i_raw[z], b_raw[z])
        hat[5, z] = dot(dot(sin_ref[...], before), sin_ref[...])
    hand_out(5)

    z_matrix = sine(nz)
    for copy in step_copies:
        copy.wait_recv()

    share = pl.ds(pl.multiple_of(slot * part, part), part)

    def slice_gain(i, carry):
        total_g, total_a = carry
        keep_g, keep_a = total_g, total_a
        mu = steps[i, 0:1, :] * lam[share, :]
        _, square, _, _, a = responses(mu)
        prefix[i, 0] = keep_g
        prefix[i, 1] = keep_a
        gains[i, 0] = square
        gains[i, 1] = a
        return square * total_g, square * total_a + a * total_g

    ones = jnp.ones((part, ny), jnp.float32)
    total_g, total_a = lax.fori_loop(0, per, slice_gain, (ones, jnp.zeros_like(ones)))
    gain_all[group, 0] = total_g
    gain_all[group, 1] = total_a
    gain_copies = []
    for d in range(1, GROUPS):
        copy = pltpu.make_async_remote_copy(
            src_ref=gain_all.at[group], dst_ref=gain_all.at[group],
            send_sem=gain_send.at[d - 1], recv_sem=gain_recv.at[d - 1],
            device_id=(lax.rem(group + d, GROUPS) * per + slot, sp), device_id_type=MESH,
        )
        copy.start()
        gain_copies.append(copy)

    for f in range(6):
        for d in range(1, spaces):
            in_copies[f * (spaces - 1) + d - 1].wait_recv()
        planes = along_z([recv[f, z] for z in range(nz)], z_matrix)
        for k in range(nz):
            spec[f, pl.ds(k * cols, cols), :] = planes[k]

    block = 32

    def pre(i, carry):
        at = pl.ds(pl.multiple_of(i * block, block), block)
        mu = step * lam[at, :]
        q = [spec[m, at, :] for m in range(4)]
        before = spec[5, at, :]
        forced, v, left, forced2 = sources(q, spec[4, at, :], before, mu)
        keep[0, at, :] = v[1]
        keep[1, at, :] = v[2]
        keep[2, at, :] = v[3]
        keep[3, at, :] = v[4]
        keep[4, at, :] = left
        keep[5, at, :] = forced2
        _, square, _, _, a = responses(mu)
        start = jnp.where(tm == 0, before, 0.0)
        fb[0, at, :] = forced + square * start
        fb[1, at, :] = forced2 + (square + a) * start
        return carry

    lax.fori_loop(0, rows // block, pre, 0)

    scan_copies = []
    for d in range(1, per):
        other = lax.rem(slot + d, per)
        copy = pltpu.make_async_remote_copy(
            src_ref=fb.at[:, pl.ds(pl.multiple_of(other * part, part), part), :],
            dst_ref=scan_in.at[slot],
            send_sem=scan_send.at[d - 1], recv_sem=scan_recv.at[d - 1],
            device_id=(group * per + other, sp), device_id_type=MESH,
        )
        copy.start()
        scan_copies.append(copy)
    scan_in[slot] = fb[:, share, :]

    def post(i, carry):
        at = pl.ds(pl.multiple_of(i * block, block), block)
        mu = step * lam[at, :]
        rho, square, v, left, a = responses(mu)
        va = [None, keep[0, at, :], keep[1, at, :], keep[2, at, :], keep[3, at, :]]
        lefta = keep[4, at, :]
        forceda = keep[5, at, :]
        beta[0, 0, at, :] = lefta
        beta[0, 1, at, :] = left
        beta[0, 2, at, :] = rho
        beta[1, 0, at, :] = forceda
        beta[1, 1, at, :] = a
        beta[1, 2, at, :] = square
        for n, m in enumerate((1, 3)):
            w = [float(x) for x in INTERP[m]]
            beta[2 + n, 0, at, :] = va[m] + w[1] * (lefta - va[2]) + w[2] * (forceda - va[4])
            beta[2 + n, 1, at, :] = v[m] - w[0] + w[1] * (left - v[2]) + w[2] * (a - v[4])
            beta[2 + n, 2, at, :] = w[0] + w[1] * rho + w[2] * square
        return carry

    lax.fori_loop(0, rows // block, post, 0)

    for copy in scan_copies:
        copy.wait_recv()
    zero = jnp.zeros((part, ny), jnp.float32)

    def advance(i, carry):
        c, d = carry
        f, b = scan_in[i, 0], scan_in[i, 1]
        scan_in[i, 0] = c
        scan_in[i, 1] = d
        g, a = gains[i, 0], gains[i, 1]
        return g * c + f, g * d + (a * c + b)

    c, d = lax.fori_loop(0, per, advance, (zero, zero))
    totals[group, 0] = c
    totals[group, 1] = d
    tot_copies = []
    for n in range(1, GROUPS):
        copy = pltpu.make_async_remote_copy(
            src_ref=totals.at[group], dst_ref=totals.at[group],
            send_sem=tot_send.at[n - 1], recv_sem=tot_recv.at[n - 1],
            device_id=(lax.rem(group + n, GROUPS) * per + slot, sp), device_id_type=MESH,
        )
        copy.start()
        tot_copies.append(copy)
    for copy in gain_copies:
        copy.wait_recv()
    for copy in tot_copies:
        copy.wait_recv()
    c, d = zero, zero
    start_c, start_d = zero, zero
    for other in range(GROUPS - 1):
        g, a = gain_all[other, 0], gain_all[other, 1]
        c, d = g * c + totals[other, 0], g * d + (a * c + totals[other, 1])
        start_c = jnp.where(group == other + 1, c, start_c)
        start_d = jnp.where(group == other + 1, d, start_d)

    for i in range(per):
        g, a = prefix[i, 0], prefix[i, 1]
        prefix[i, 0] = scan_in[i, 0] + g * start_c
        prefix[i, 1] = scan_in[i, 1] + (g * start_d + a * start_c)

    back_copies = []
    for d in range(1, per):
        other = lax.rem(slot + d, per)
        copy = pltpu.make_async_remote_copy(
            src_ref=prefix.at[other], dst_ref=cd.at[:, share, :],
            send_sem=back_send.at[d - 1], recv_sem=back_recv.at[d - 1],
            device_id=(group * per + other, sp), device_id_type=MESH,
        )
        copy.start()
        back_copies.append(copy)
    cd[:, share, :] = prefix[slot]
    for copy in back_copies:
        copy.wait_recv()

    out_copies = []
    for m in (0, 4, 2, 1, 3):
        for r in range(0, cols, 8):
            planes = []
            for k in range(nz):
                at = pl.ds(k * cols + r, 8)
                before = spec[5, at, :]
                c = jnp.where(tm == 0, before, cd[0, at, :])
                d = jnp.where(tm == 0, before, cd[1, at, :])
                if m == 0:
                    planes.append(d)
                else:
                    n = {2: 0, 4: 1, 1: 2, 3: 3}[m]
                    planes.append(beta[n, 0, at, :] + beta[n, 1, at, :] * c + beta[n, 2, at, :] * d)
            planes = along_z(planes, z_matrix)
            for z in range(nz):
                spec_at = pl.ds(z * cols + r, 8)
                yout[m, spec_at, :] = planes[z]
        yout[m] = dot(yout[m], sin_ref[...])
        mine = pl.ds(pl.multiple_of(sp * cols, cols), cols)
        for d in range(1, spaces):
            other = lax.rem(sp + d, spaces)
            for z in range(depth):
                copy = pltpu.make_async_remote_copy(
                    src_ref=yout.at[m, pl.ds(pl.multiple_of((other * depth + z) * cols, cols), cols), :],
                    dst_ref=outr.at[m, z, mine, :],
                    send_sem=out_send.at[m, d - 1, z], recv_sem=out_recv.at[m, d - 1, z],
                    device_id=(tm, other), device_id_type=MESH,
                )
                copy.start()
                out_copies.append(copy)
        for z in range(depth):
            outr[m, z, mine, :] = yout[m, pl.ds(pl.multiple_of((sp * depth + z) * cols, cols), cols), :]

    stores = []
    each = (spaces - 1) * depth
    for n, m in enumerate((0, 4, 2, 1, 3)):
        for copy in out_copies[n * each : (n + 1) * each]:
            copy.wait_recv()
        for z in range(depth):
            res[m, z] = dot(sin_ref[...], outr[m, z])
        store = pltpu.make_async_copy(res.at[m], out_hbm.at[0, m], store_sem.at[m])
        store.start()
        stores.append(store)
    for copy in [shift] + step_copies + in_copies + gain_copies + scan_copies + tot_copies + back_copies + out_copies:
        copy.wait_send()
    for store in stores:
        store.wait()


def body(sizes, initial, start_guess, forcing, step_size):
    count, spaces, nx, ny, nz = sizes
    per = count // GROUPS
    depth = nz // spaces
    cols = nx // spaces
    rows = nz * cols
    part = rows // per
    table = jnp.asarray(sine(nx), jnp.float32)
    lamxy = jnp.asarray(eigen(nx)[:, None] + eigen(ny)[None, :], jnp.float32)
    vmem = pl.BlockSpec(memory_space=pltpu.VMEM)
    hbm = pl.BlockSpec(memory_space=pl.ANY)
    f32 = lambda *shape: pltpu.VMEM(shape, jnp.float32)
    dma = lambda *shape: pltpu.SemaphoreType.DMA(shape)
    return pl.pallas_call(
        functools.partial(kernel, sizes),
        out_shape=jax.ShapeDtypeStruct((1, 5, depth, nx, ny), jnp.float32),
        in_specs=[hbm, hbm, hbm, pl.BlockSpec(memory_space=pltpu.SMEM), vmem, vmem],
        out_specs=hbm,
        scratch_shapes=[
            f32(5, depth, nx, ny), f32(depth, nx, ny), f32(depth, nx, ny), f32(depth, nx, ny),
            f32(6, depth, nx, ny), f32(6, nz, cols, ny), f32(rows, ny), f32(6, rows, ny),
            f32(2, rows, ny), f32(6, rows, ny), f32(per, 8, ny), f32(per, 2, part, ny),
            f32(per, 2, part, ny), f32(GROUPS, 2, part, ny), f32(per, 2, part, ny),
            f32(GROUPS, 2, part, ny), f32(2, rows, ny), f32(4, 3, rows, ny), f32(5, rows, ny),
            f32(5, depth, nx, ny), f32(5, depth, nx, ny),
            dma(3), dma(5), dma(6, spaces - 1), dma(6, spaces - 1), dma(2), dma(per - 1), dma(per - 1),
            dma(per - 1), dma(per - 1), dma(GROUPS - 1), dma(GROUPS - 1), dma(GROUPS - 1), dma(GROUPS - 1),
            dma(per - 1), dma(per - 1), dma(5, spaces - 1, depth), dma(5, spaces - 1, depth),
        ],
        compiler_params=pltpu.CompilerParams(collective_id=0, has_side_effects=True),
    )(start_guess, forcing, initial, step_size, table, lamxy)


def solution(mesh):
    sizes = (mesh.shape["tm"], mesh.shape["space"], 128, 128, 8)
    placed = (
        P("space", None, None),
        P("tm", "space", None, None),
        P("tm", None, "space", None, None),
        P("tm"),
    )
    return jax.shard_map(
        functools.partial(body, sizes),
        mesh=mesh,
        in_specs=placed,
        out_specs=P("tm", None, "space", None, None),
        check_vma=False,
    )
```

```python
import functools
import math

import jax
import jax.numpy as jnp
import numpy as np
from jax import lax
from jax.experimental import pallas as pl
from jax.experimental.pallas import tpu as pltpu
from jax.sharding import PartitionSpec as P

MESH = pl.DeviceIdType.MESH
GROUPS = 4
RING = 8
PLANES = 8
SPACES = 4
OWNERS = 2 * SPACES
DEPTH = PLANES // SPACES
WIDTH = 128
COLS = WIDTH // OWNERS
SUB = 8
CHUNKS = COLS // SUB
ROWS = PLANES * SUB


def node_tables():
    radical = math.sqrt(3.0 / 7.0)
    times = [0.0, (1.0 - radical) / 2.0, 0.5, (1.0 + radical) / 2.0, 1.0]
    integrals = np.zeros((4, 5))
    for column in range(5):
        coeffs = np.array([1.0])
        for other in range(5):
            if other != column:
                coeffs = np.convolve(coeffs, [-times[other], 1.0]) / (times[column] - times[other])
        powers = np.arange(1, 6)
        for section in range(4):
            integrals[section, column] = np.sum(
                coeffs * (times[section + 1] ** powers - times[section] ** powers) / powers
            )
    coarse = [0.0, 0.5, 1.0]
    interp = np.zeros((5, 3))
    for column in range(3):
        for section in range(5):
            weight = 1.0
            for other in range(3):
                if other != column:
                    weight *= (times[section] - coarse[other]) / (coarse[column] - coarse[other])
            interp[section, column] = weight
    return times, integrals, interp


TIMES, QUAD, INTERP = node_tables()
SPACING = [TIMES[m + 1] - TIMES[m] for m in range(4)]


def mixed(weights, values):
    total = None
    for weight, value in zip(weights, values):
        if value is None or abs(weight) < 1e-14:
            continue
        term = float(weight) * value
        total = term if total is None else total + term
    return total


def sweep(u, q, mu):
    v = [u[0]]
    for m in range(4):
        weights = list(QUAD[m])
        weights[m] -= SPACING[m]
        rate = mixed(weights + [SPACING[m]], u + [v[m]])
        new = -mu * rate
        if q is not None:
            new = new + q[m]
        if v[m] is not None:
            new = new + v[m]
        v.append(new)
    return v


def coarse_terms(v, q, mu):
    weights = QUAD[0] + QUAD[1]
    weights[0] -= 0.5
    left = -mu * mixed(weights, v)
    weights = QUAD[2] + QUAD[3]
    weights[2] -= 0.5
    right = -mu * mixed(weights, v)
    if q is not None:
        left = left + (q[0] + q[1])
        right = right + (q[2] + q[3])
    return left, right


def sources(q, guess, before, mu):
    rho = 1.0 - 0.5 * mu
    v = sweep([before, guess, guess, guess, guess], q, mu)
    left, right = coarse_terms(v, q, mu)
    forced = rho * left + right
    u = [None, None, left, None, forced]
    for m in (1, 3):
        u[m] = v[m] + mixed(INTERP[m], [-before, left - v[2], forced - v[4]])
    v = sweep(u, q, mu)
    left2, right2 = coarse_terms(v, q, mu)
    return forced, v, left2, rho * left2 + right2


def responses(mu):
    rho = 1.0 - 0.5 * mu
    square = rho * rho
    u = [1.0, None, rho, None, square]
    for m in (1, 3):
        u[m] = float(INTERP[m, 0]) + float(INTERP[m, 1]) * rho + float(INTERP[m, 2]) * square
    v = sweep(u, None, mu)
    left, right = coarse_terms(v, None, mu)
    return rho, square, v, left, rho * left + right


def sine(length):
    k = np.arange(1, length + 1)
    return math.sqrt(2.0 / (length + 1)) * np.sin(math.pi / (length + 1) * np.outer(k, k))


def eigen(length):
    return 2.0 - 2.0 * np.cos(math.pi / (length + 1) * np.arange(1, length + 1))


def along_z(planes, matrix):
    n = len(planes)
    half = n // 2
    even = [planes[i] + planes[n - 1 - i] for i in range(half)]
    odd = [planes[i] - planes[n - 1 - i] for i in range(half)]
    out = []
    for k in range(n):
        out.append(mixed(matrix[k][:half], even if k % 2 == 0 else odd))
    return out


def kernel(
    start_hbm, force_hbm, first_hbm, step_ref, sin_hbm, lamxy_hbm, out_ref,
    f_raw, g_raw, i_raw, sin_ref, lamxy, hat, gin, qin, firsts, ghat, qhat, shifted, lam, tab, alpha,
    pair_steps, all_steps, gains, gain_all, fb, scan_in, totals, back, cd, cd_odd, yout, outr,
    load_sem, g_send, g_recv, q_send, q_recv, r_send, r_recv, i_send, i_recv, shift_sem,
    pstep_sem, step_send, step_recv, scan_send, scan_recv, gain_send, gain_recv, tot_send, tot_recv,
    back_send, back_recv, o_send, o_recv, m_send, m_recv,
):
    high = lax.Precision.HIGHEST
    tm = lax.axis_index("tm")
    sp = lax.axis_index("space")
    pair, half = tm // 2, tm % 2
    group, slot = pair // RING, pair % RING
    own = half * SPACES + sp

    def dot(a, b):
        return jnp.dot(a, b, precision=high, preferred_element_type=jnp.float32)

    def owner(d):
        other = lax.rem(own + d, OWNERS)
        return other, (pair * 2 + other // SPACES, lax.rem(other, SPACES))

    def along_ring(d):
        other = lax.rem(slot + d, RING)
        return other, ((group * RING + other) * 2 + half, sp)

    def across(d):
        return ((lax.rem(group + d, GROUPS) * RING + slot) * 2 + half, sp)

    def send(src, dst, send_sem, recv_sem, target):
        copy = pltpu.make_async_remote_copy(
            src_ref=src, dst_ref=dst, send_sem=send_sem, recv_sem=recv_sem,
            device_id=target, device_id_type=MESH,
        )
        copy.start()
        return copy

    pairs = GROUPS * RING
    following = (lax.rem(pair + 1, pairs) * 2 + half, sp)
    preceding = (lax.rem(pair + pairs - 1, pairs) * 2 + half, sp)
    partner = (pair * 2 + 1 - half, lax.rem(sp + SPACES // 2, SPACES))

    loads = [
        pltpu.make_async_copy(start_hbm.at[0], g_raw, load_sem.at[0]),
        pltpu.make_async_copy(sin_hbm, sin_ref, load_sem.at[1]),
        pltpu.make_async_copy(force_hbm.at[0], f_raw, load_sem.at[2]),
        pltpu.make_async_copy(lamxy_hbm.at[pl.ds(pl.multiple_of(own * COLS, COLS), COLS)], lamxy, load_sem.at[3]),
        pltpu.make_async_copy(first_hbm, i_raw, load_sem.at[4]),
    ]
    for load in loads:
        load.start()

    barrier = pltpu.get_barrier_semaphore()

    def greet(target):
        pl.semaphore_signal(barrier, inc=1, device_id=target, device_id_type=MESH)

    for d in range(1, OWNERS):
        greet(owner(d)[1])
    for d in range(1, RING):
        greet(along_ring(d)[1])
    for d in range(1, GROUPS):
        greet(across(d))
    greet(following)
    greet(preceding)

    step = step_ref[0]
    pair_steps[half] = jnp.full((SUB, WIDTH), step, jnp.float32)
    loads[0].wait()
    loads[1].wait()

    def transform(f, planes):
        for z in range(DEPTH):
            hat[f, z] = dot(dot(sin_ref[...], planes[z]), sin_ref[...])

    transform(4, [g_raw[z] for z in range(DEPTH)])
    loads[2].wait()
    pl.semaphore_wait(barrier, OWNERS + RING + GROUPS - 1)

    mine = pl.ds(pl.multiple_of(own * COLS, COLS), COLS)
    here = pl.ds(sp * DEPTH, DEPTH)

    def slab(other, first, size):
        return pl.ds(pl.multiple_of(other * COLS + first, SUB), size)

    pstep_copy = send(
        pair_steps.at[half], pair_steps.at[half], pstep_sem.at[0], pstep_sem.at[1], partner
    )
    g_copies = []
    for d in range(1, OWNERS):
        other, target = owner(d)
        g_copies.append(send(
            hat.at[4, :, slab(other, 0, COLS), :], gin.at[half, here],
            g_send.at[d - 1], g_recv.at[d - 1], target,
        ))
    gin[half, here] = hat[4, :, mine, :]
    q_copies = []
    for m in range(4):
        planes = [
            step * mixed(QUAD[m], [f_raw[j, z] for j in range(5)]) for z in range(DEPTH)
        ]
        transform(m, planes)
        for d in range(1, OWNERS):
            other, target = owner(d)
            q_copies.append(send(
                hat.at[m, :, slab(other, 0, SUB), :], qin.at[0, half, m, here],
                q_send.at[m, d - 1], q_recv.at[m, d - 1], target,
            ))
    r_copies = []
    for d in range(1, OWNERS):
        other, target = owner(d)
        r_copies.append(send(
            hat.at[pl.ds(0, 4), :, slab(other, SUB, SUB), :], qin.at[1, half, :, here],
            r_send.at[d - 1], r_recv.at[d - 1], target,
        ))
    for h in range(CHUNKS):
        for m in range(4):
            qin[h, half, m, here] = hat[m, :, slab(own, h * SUB, SUB), :]

    for load in loads[3:]:
        load.wait()

    def first_copy(d):
        other = lax.rem(sp + d, SPACES)
        return pltpu.make_async_remote_copy(
            src_ref=hat.at[5, :, slab(half * SPACES + other, 0, COLS), :],
            dst_ref=firsts.at[here], send_sem=i_send.at[d - 1], recv_sem=i_recv.at[d - 1],
            device_id=(tm, other), device_id_type=MESH,
        )

    @pl.when(pair == 0)
    def _():
        transform(5, [i_raw[z] for z in range(DEPTH)])
        for d in range(1, SPACES):
            first_copy(d).start()
        firsts[here] = hat[5, :, mine, :]

    z_matrix = sine(PLANES)
    z_eigen = eigen(PLANES)
    for h in range(CHUNKS):
        for k in range(PLANES):
            lam[h, pl.ds(k * SUB, SUB), :] = lamxy[pl.ds(h * SUB, SUB), :] + float(z_eigen[k])

    pstep_copy.wait_recv()
    step_copies = []
    for d in range(1, RING):
        _, target = along_ring(d)
        step_copies.append(send(
            pair_steps, all_steps.at[slot], step_send.at[d - 1], step_recv.at[d - 1], target
        ))
    all_steps[slot] = pair_steps[...]

    def table(i, carry):
        at = pl.ds(pl.multiple_of(i * 2 * SUB, 2 * SUB), 2 * SUB)
        for h in range(CHUNKS):
            for s in range(2):
                mu = pair_steps[s, 0:1, :] * lam[h, at, :]
                rho, square, v, left, a = responses(mu)
                tab[h, s, 0, at, :] = left
                tab[h, s, 1, at, :] = rho
                tab[h, s, 2, at, :] = a
                tab[h, s, 3, at, :] = square
                for n, m in enumerate((1, 3)):
                    w = [float(x) for x in INTERP[m]]
                    tab[h, s, 4 + 2 * n, at, :] = v[m] - w[0] + w[1] * (left - v[2]) + w[2] * (a - v[4])
                    tab[h, s, 5 + 2 * n, at, :] = w[0] + w[1] * rho + w[2] * square
        return carry

    lax.fori_loop(0, ROWS // (2 * SUB), table, 0)

    for copy in g_copies:
        copy.wait_recv()
    for s in (1, 0):
        for h in range(CHUNKS):
            planes = along_z([gin[s, z, pl.ds(h * SUB, SUB), :] for z in range(PLANES)], z_matrix)
            for k in range(PLANES):
                ghat[s, h, pl.ds(k * SUB, SUB), :] = planes[k]
        if s == 1:
            shift_copy = send(ghat.at[1], shifted, shift_sem.at[0], shift_sem.at[1], following)

    for copy in step_copies:
        copy.wait_recv()
    share = pl.ds(pl.multiple_of(slot * SUB, SUB), SUB)

    def pair_gain(i, carry):
        out = []
        for h in range(CHUNKS):
            total_g, total_a = carry[h]
            gains[i, 2, h] = total_g
            gains[i, 3, h] = total_a
            _, g0, _, _, a0 = responses(all_steps[i, 0, 0:1, :] * lam[h, share, :])
            _, g1, _, _, a1 = responses(all_steps[i, 1, 0:1, :] * lam[h, share, :])
            g, a = g1 * g0, g1 * a0 + a1 * g0
            gains[i, 0, h] = g
            gains[i, 1, h] = a
            out.append((g * total_g, g * total_a + a * total_g))
        return tuple(out)

    ones = jnp.ones((SUB, WIDTH), jnp.float32)
    zero = jnp.zeros((SUB, WIDTH), jnp.float32)
    ends = lax.fori_loop(0, RING, pair_gain, ((ones, zero),) * CHUNKS)
    for h in range(CHUNKS):
        gain_all[group, 0, h] = ends[h][0]
        gain_all[group, 1, h] = ends[h][1]
    gain_copies = [
        send(gain_all.at[group], gain_all.at[group], gain_send.at[d - 1], gain_recv.at[d - 1], across(d))
        for d in range(1, GROUPS)
    ]

    def pre(h):
        def step_pre(i, carry):
            two = pl.ds(pl.multiple_of(i * 2 * SUB, 2 * SUB), 2 * SUB)
            forced, extra = [], []
            for s in range(2):
                mu = pair_steps[s, 0:1, :] * lam[h, two, :]
                before = shifted[h, two, :] if s == 0 else ghat[0, h, two, :]
                f, v, left, b = sources([qhat[s, m, two, :] for m in range(4)], ghat[s, h, two, :], before, mu)
                alpha[h, s, 0, two, :] = left
                alpha[h, s, 1, two, :] = b
                for n, m in enumerate((1, 3)):
                    w = [float(x) for x in INTERP[m]]
                    alpha[h, s, 2 + n, two, :] = v[m] + w[1] * (left - v[2]) + w[2] * (b - v[4])
                if s == 0:
                    alpha[h, 0, 4, two, :] = f
                    begin = jnp.where(pair == 0, before, 0.0)
                    square, a = tab[h, 0, 3, two, :], tab[h, 0, 2, two, :]
                    f = f + square * begin
                    b = b + (square + a) * begin
                forced.append(f)
                extra.append(b)
            square, a = tab[h, 1, 3, two, :], tab[h, 1, 2, two, :]
            f = square * forced[0] + forced[1]
            b = square * extra[0] + (a * forced[0] + extra[1])
            for n in range(2):
                fb[h, 2 * i + n, 0] = f[n * SUB : (n + 1) * SUB]
                fb[h, 2 * i + n, 1] = b[n * SUB : (n + 1) * SUB]
            return carry

        lax.fori_loop(0, ROWS // (2 * SUB), step_pre, 0)

    scan_copies = []
    for h in range(CHUNKS):
        if h == 0:
            for copy in q_copies:
                copy.wait_recv()
        else:
            for copy in r_copies:
                copy.wait_recv()
        for s in range(2):
            for m in range(4):
                planes = along_z([qin[h, s, m, z] for z in range(PLANES)], z_matrix)
                for k in range(PLANES):
                    qhat[s, m, pl.ds(k * SUB, SUB), :] = planes[k]
        if h == 0:
            shift_copy.wait_recv()

            @pl.when(pair == 0)
            def _():
                for d in range(1, SPACES):
                    first_copy(d).wait_recv()
                for n in range(CHUNKS):
                    planes = along_z([firsts[z, pl.ds(n * SUB, SUB), :] for z in range(PLANES)], z_matrix)
                    for k in range(PLANES):
                        shifted[n, pl.ds(k * SUB, SUB), :] = planes[k]

        pre(h)
        for d in range(1, RING):
            other, target = along_ring(d)
            scan_copies.append(send(
                fb.at[h, other], scan_in.at[h, slot], scan_send.at[h, d - 1], scan_recv.at[h, d - 1], target
            ))
        scan_in[h, slot] = fb[h, slot]

    tot_copies = []
    for h in range(CHUNKS):
        for copy in scan_copies[h * (RING - 1) : (h + 1) * (RING - 1)]:
            copy.wait_recv()
        c, d = zero, zero
        for i in range(RING):
            f, b = scan_in[h, i, 0], scan_in[h, i, 1]
            back[h, i, 0] = c
            back[h, i, 1] = d
            g, a = gains[i, 0, h], gains[i, 1, h]
            c, d = g * c + f, g * d + (a * c + b)
        totals[h, group, 0] = c
        totals[h, group, 1] = d
        for n in range(1, GROUPS):
            tot_copies.append(send(
                totals.at[h, group], totals.at[h, group],
                tot_send.at[h, n - 1], tot_recv.at[h, n - 1], across(n),
            ))
    for copy in gain_copies:
        copy.wait_recv()
    back_copies = []
    for h in range(CHUNKS):
        for copy in tot_copies[h * (GROUPS - 1) : (h + 1) * (GROUPS - 1)]:
            copy.wait_recv()
        c, d = zero, zero
        start_c, start_d = zero, zero
        for other in range(GROUPS - 1):
            g, a = gain_all[other, 0, h], gain_all[other, 1, h]
            c, d = g * c + totals[h, other, 0], g * d + (a * c + totals[h, other, 1])
            start_c = jnp.where(group == other + 1, c, start_c)
            start_d = jnp.where(group == other + 1, d, start_d)
        for i in range(RING):
            g, a = gains[i, 2, h], gains[i, 3, h]
            back[h, i, 0] = back[h, i, 0] + g * start_c
            back[h, i, 1] = back[h, i, 1] + (g * start_d + a * start_c)
        for n in range(1, RING):
            other, target = along_ring(n)
            back_copies.append(send(
                back.at[h, other], cd.at[h, slot], back_send.at[h, n - 1], back_recv.at[h, n - 1], target
            ))
        cd[h, slot] = back[h, slot]

    order = (0, 4, 2, 1, 3)
    o_copies, m_copies = [], []
    for h in range(CHUNKS):
        for copy in back_copies[h * (RING - 1) : (h + 1) * (RING - 1)]:
            copy.wait_recv()
        for k in range(PLANES):
            at = pl.ds(k * SUB, SUB)
            before = shifted[h, at, :]
            c = jnp.where(pair == 0, before, cd[h, k, 0])
            d = jnp.where(pair == 0, before, cd[h, k, 1])
            g, a = tab[h, 0, 3, at, :], tab[h, 0, 2, at, :]
            cd[h, k, 0] = c
            cd[h, k, 1] = d
            cd_odd[h, k, 0] = g * c + alpha[h, 0, 4, at, :]
            cd_odd[h, k, 1] = g * d + (a * c + alpha[h, 0, 1, at, :])
        for m in order:
            for s in range(2):
                src = cd if s == 0 else cd_odd
                planes = []
                for k in range(PLANES):
                    at = pl.ds(k * SUB, SUB)
                    if m == 0:
                        planes.append(src[h, k, 1])
                    else:
                        n = {2: 0, 4: 1, 1: 2, 3: 3}[m]
                        planes.append(
                            alpha[h, s, n, at, :]
                            + (tab[h, s, 2 * n, at, :] * src[h, k, 0] + tab[h, s, 2 * n + 1, at, :] * src[h, k, 1])
                        )
                planes = along_z(planes, z_matrix)
                for z in range(PLANES):
                    yout[h, m, s, z] = planes[z]
            rows = yout[h, m].reshape(2 * ROWS, WIDTH)
            yout[h, m] = dot(rows, sin_ref[...]).reshape(2, PLANES, SUB, WIDTH)
            if h == CHUNKS - 1:
                for d in range(1, OWNERS):
                    other, target = owner(d)
                    m_copies.append(send(
                        yout.at[h, m, other // SPACES, pl.ds(lax.rem(other, SPACES) * DEPTH, DEPTH)],
                        outr.at[m, :, slab(own, h * SUB, SUB), :],
                        m_send.at[m, d - 1], m_recv.at[m, d - 1], target,
                    ))
            outr[m, :, slab(own, h * SUB, SUB), :] = yout[h, m, half, here]
        if h < CHUNKS - 1:
            for d in range(1, OWNERS):
                other, target = owner(d)
                o_copies.append(send(
                    yout.at[h, :, other // SPACES, pl.ds(lax.rem(other, SPACES) * DEPTH, DEPTH)],
                    outr.at[:, :, slab(own, h * SUB, SUB), :],
                    o_send.at[h, d - 1], o_recv.at[h, d - 1], target,
                ))

    for copy in o_copies:
        copy.wait_recv()
    for n, m in enumerate(order):
        for copy in m_copies[n * (OWNERS - 1) : (n + 1) * (OWNERS - 1)]:
            copy.wait_recv()
        for z in range(DEPTH):
            out_ref[0, m, z] = dot(sin_ref[...], outr[m, z])

    for copy in (
        [pstep_copy, shift_copy] + g_copies + q_copies + r_copies + step_copies + gain_copies
        + scan_copies + tot_copies + back_copies + o_copies + m_copies
    ):
        copy.wait_send()

    @pl.when(pair == 0)
    def _():
        for d in range(1, SPACES):
            first_copy(d).wait_send()


def body(initial, start_guess, forcing, step_size):
    table = jnp.asarray(sine(WIDTH), jnp.float32)
    lamxy = jnp.asarray(eigen(WIDTH)[:, None] + eigen(WIDTH)[None, :], jnp.float32)
    hbm = pl.BlockSpec(memory_space=pl.ANY)
    f32 = lambda *shape: pltpu.VMEM(shape, jnp.float32)
    dma = lambda *shape: pltpu.SemaphoreType.DMA(shape)
    tile = (SUB, WIDTH)
    return pl.pallas_call(
        kernel,
        out_shape=jax.ShapeDtypeStruct((1, 5, DEPTH, WIDTH, WIDTH), jnp.float32),
        in_specs=[hbm, hbm, hbm, pl.BlockSpec(memory_space=pltpu.SMEM), hbm, hbm],
        out_specs=pl.BlockSpec(memory_space=pltpu.VMEM),
        scratch_shapes=[
            f32(5, DEPTH, WIDTH, WIDTH), f32(DEPTH, WIDTH, WIDTH), f32(DEPTH, WIDTH, WIDTH),
            f32(WIDTH, WIDTH), f32(COLS, WIDTH), f32(6, DEPTH, WIDTH, WIDTH),
            f32(2, PLANES, COLS, WIDTH), f32(CHUNKS, 2, 4, PLANES, *tile), f32(PLANES, COLS, WIDTH),
            f32(2, CHUNKS, ROWS, WIDTH), f32(2, 4, ROWS, WIDTH), f32(CHUNKS, ROWS, WIDTH),
            f32(CHUNKS, ROWS, WIDTH), f32(CHUNKS, 2, 8, ROWS, WIDTH), f32(CHUNKS, 2, 5, ROWS, WIDTH),
            f32(2, *tile), f32(RING, 2, *tile), f32(RING, 4, CHUNKS, *tile), f32(GROUPS, 2, CHUNKS, *tile),
            f32(CHUNKS, RING, 2, *tile), f32(CHUNKS, RING, 2, *tile), f32(CHUNKS, GROUPS, 2, *tile),
            f32(CHUNKS, RING, 2, *tile), f32(CHUNKS, RING, 2, *tile), f32(CHUNKS, RING, 2, *tile),
            f32(CHUNKS, 5, 2, PLANES, *tile), f32(5, DEPTH, WIDTH, WIDTH),
            dma(5), dma(OWNERS - 1), dma(OWNERS - 1), dma(4, OWNERS - 1), dma(4, OWNERS - 1),
            dma(OWNERS - 1), dma(OWNERS - 1), dma(SPACES - 1), dma(SPACES - 1), dma(2),
            dma(2), dma(RING - 1), dma(RING - 1), dma(CHUNKS, RING - 1), dma(CHUNKS, RING - 1),
            dma(GROUPS - 1), dma(GROUPS - 1), dma(CHUNKS, GROUPS - 1), dma(CHUNKS, GROUPS - 1),
            dma(CHUNKS, RING - 1), dma(CHUNKS, RING - 1), dma(CHUNKS, OWNERS - 1), dma(CHUNKS, OWNERS - 1),
            dma(5, OWNERS - 1), dma(5, OWNERS - 1),
        ],
        compiler_params=pltpu.CompilerParams(collective_id=0, has_side_effects=True),
    )(start_guess, forcing, initial, step_size, table, lamxy)


def solution(mesh):
    placed = (
        P("space", None, None),
        P("tm", "space", None, None),
        P("tm", None, "space", None, None),
        P("tm"),
    )
    return jax.shard_map(
        body,
        mesh=mesh,
        in_specs=placed,
        out_specs=P("tm", None, "space", None, None),
        check_vma=False,
    )
```

```python
import functools
import math

import jax
import jax.numpy as jnp
import numpy as np
from jax import lax
from jax.experimental import pallas as pl
from jax.experimental.pallas import tpu as pltpu
from jax.sharding import PartitionSpec as P

MESH = pl.DeviceIdType.MESH
GROUPS = 4
RING = 8
PLANES = 8
SPACES = 4
OWNERS = 2 * SPACES
DEPTH = PLANES // SPACES
WIDTH = 128
COLS = WIDTH // OWNERS
SUB = 8
CHUNKS = COLS // SUB
ROWS = PLANES * SUB

GUESS, FIRST, SHIFT, PSTEP, STEPS, GAINS, OUT = range(7)
FIELDS, SCAN, TOTALS, BACK = (7 + n * CHUNKS for n in range(4))
LAST = 7 + 4 * CHUNKS
PHASES = LAST + 5


def node_tables():
    radical = math.sqrt(3.0 / 7.0)
    times = [0.0, (1.0 - radical) / 2.0, 0.5, (1.0 + radical) / 2.0, 1.0]
    integrals = np.zeros((4, 5))
    for column in range(5):
        coeffs = np.array([1.0])
        for other in range(5):
            if other != column:
                coeffs = np.convolve(coeffs, [-times[other], 1.0]) / (times[column] - times[other])
        powers = np.arange(1, 6)
        for section in range(4):
            integrals[section, column] = np.sum(
                coeffs * (times[section + 1] ** powers - times[section] ** powers) / powers
            )
    coarse = [0.0, 0.5, 1.0]
    interp = np.zeros((5, 3))
    for column in range(3):
        for section in range(5):
            weight = 1.0
            for other in range(3):
                if other != column:
                    weight *= (times[section] - coarse[other]) / (coarse[column] - coarse[other])
            interp[section, column] = weight
    return times, integrals, interp


TIMES, QUAD, INTERP = node_tables()
SPACING = [TIMES[m + 1] - TIMES[m] for m in range(4)]


def mixed(weights, values):
    total = None
    for weight, value in zip(weights, values):
        if value is None or abs(weight) < 1e-14:
            continue
        term = float(weight) * value
        total = term if total is None else total + term
    return total


def sweep(u, q, mu):
    v = [u[0]]
    for m in range(4):
        weights = list(QUAD[m])
        weights[m] -= SPACING[m]
        rate = mixed(weights + [SPACING[m]], u + [v[m]])
        new = -mu * rate
        if q is not None:
            new = new + q[m]
        if v[m] is not None:
            new = new + v[m]
        v.append(new)
    return v


def coarse_terms(v, q, mu):
    weights = QUAD[0] + QUAD[1]
    weights[0] -= 0.5
    left = -mu * mixed(weights, v)
    weights = QUAD[2] + QUAD[3]
    weights[2] -= 0.5
    right = -mu * mixed(weights, v)
    if q is not None:
        left = left + (q[0] + q[1])
        right = right + (q[2] + q[3])
    return left, right


def sources(q, guess, before, mu):
    rho = 1.0 - 0.5 * mu
    v = sweep([before, guess, guess, guess, guess], q, mu)
    left, right = coarse_terms(v, q, mu)
    forced = rho * left + right
    u = [None, None, left, None, forced]
    for m in (1, 3):
        u[m] = v[m] + mixed(INTERP[m], [-before, left - v[2], forced - v[4]])
    v = sweep(u, q, mu)
    left2, right2 = coarse_terms(v, q, mu)
    return forced, v, left2, rho * left2 + right2


def responses(mu):
    rho = 1.0 - 0.5 * mu
    square = rho * rho
    u = [1.0, None, rho, None, square]
    for m in (1, 3):
        u[m] = float(INTERP[m, 0]) + float(INTERP[m, 1]) * rho + float(INTERP[m, 2]) * square
    v = sweep(u, None, mu)
    left, right = coarse_terms(v, None, mu)
    return rho, square, v, left, rho * left + right


def sine(length):
    k = np.arange(1, length + 1)
    return math.sqrt(2.0 / (length + 1)) * np.sin(math.pi / (length + 1) * np.outer(k, k))


def eigen(length):
    return 2.0 - 2.0 * np.cos(math.pi / (length + 1) * np.arange(1, length + 1))


def along_z(planes, matrix):
    n = len(planes)
    half = n // 2
    even = [planes[i] + planes[n - 1 - i] for i in range(half)]
    odd = [planes[i] - planes[n - 1 - i] for i in range(half)]
    out = []
    for k in range(n):
        out.append(mixed(matrix[k][:half], even if k % 2 == 0 else odd))
    return out


def kernel(
    start_hbm, force_hbm, first_hbm, step_ref, sin_hbm, lamxy_hbm, out_ref,
    f_raw, g_raw, i_raw, sin_ref, lamxy, sin_hi, sin_lo, hat, gin, qin, firsts, ghat, qhat,
    shifted, lam, tab, alpha, pair_steps, all_steps, gains, gain_all, fb, scan_in, totals, back, cd,
    cd_odd, yout, outr, measure, load_sem, send_sem, recv_sem,
):
    tm = lax.axis_index("tm")
    sp = lax.axis_index("space")
    pair, half = tm // 2, tm % 2
    group, slot = pair // RING, pair % RING
    own = half * SPACES + sp

    def halves(x):
        hi = x.astype(jnp.bfloat16)
        return hi, (x - hi.astype(jnp.float32)).astype(jnp.bfloat16)

    def product(a, b):
        dot = functools.partial(jnp.dot, preferred_element_type=jnp.float32)
        return dot(a[0], b[0]) + (dot(a[0], b[1]) + dot(a[1], b[0]))

    def matrix():
        return sin_hi[...], sin_lo[...]

    def owner(d):
        other = lax.rem(own + d, OWNERS)
        return other, (pair * 2 + other // SPACES, lax.rem(other, SPACES))

    def along_ring(d):
        other = lax.rem(slot + d, RING)
        return other, ((group * RING + other) * 2 + half, sp)

    def across(d):
        return ((lax.rem(group + d, GROUPS) * RING + slot) * 2 + half, sp)

    sent = {}

    def tiles(ref):
        return math.prod(ref.shape) // (SUB * WIDTH)

    def describe(src, dst, phase, target):
        return pltpu.make_async_remote_copy(
            src_ref=src, dst_ref=dst, send_sem=send_sem.at[phase], recv_sem=recv_sem.at[phase],
            device_id=target, device_id_type=MESH,
        )

    def send(src, dst, phase, target):
        describe(src, dst, phase, target).start()
        sent[phase] = sent.get(phase, 0) + tiles(src)

    def settle(sem, count):
        some = measure.at[pl.ds(0, count)]
        pltpu.make_async_copy(some, some, sem).wait()

    def arrived(phase):
        settle(recv_sem.at[phase], sent[phase])

    pairs = GROUPS * RING
    following = (lax.rem(pair + 1, pairs) * 2 + half, sp)
    preceding = (lax.rem(pair + pairs - 1, pairs) * 2 + half, sp)
    partner = (pair * 2 + 1 - half, lax.rem(sp + SPACES // 2, SPACES))

    loads = [
        pltpu.make_async_copy(start_hbm.at[0], g_raw, load_sem.at[0]),
        pltpu.make_async_copy(sin_hbm, sin_ref, load_sem.at[1]),
        pltpu.make_async_copy(force_hbm.at[0], f_raw, load_sem.at[2]),
        pltpu.make_async_copy(lamxy_hbm.at[pl.ds(pl.multiple_of(own * COLS, COLS), COLS)], lamxy, load_sem.at[3]),
        pltpu.make_async_copy(first_hbm, i_raw, load_sem.at[4]),
    ]
    for load in loads:
        load.start()

    barrier = pltpu.get_barrier_semaphore()

    def greet(target):
        pl.semaphore_signal(barrier, inc=1, device_id=target, device_id_type=MESH)

    for d in range(1, OWNERS):
        greet(owner(d)[1])
    for d in range(1, RING):
        greet(along_ring(d)[1])
    for d in range(1, GROUPS):
        greet(across(d))
    greet(following)
    greet(preceding)

    for load in loads[:2]:
        load.wait()
    step = step_ref[0]
    pair_steps[half] = jnp.full((SUB, WIDTH), step, jnp.float32)
    sin_hi[...], sin_lo[...] = halves(sin_ref[...])

    def transform(f, planes):
        wide = product(matrix(), halves(jnp.concatenate(planes, axis=1)))
        tall = jnp.concatenate([wide[:, z * WIDTH : (z + 1) * WIDTH] for z in range(DEPTH)], axis=0)
        hat[f] = product(halves(tall), matrix()).reshape(DEPTH, WIDTH, WIDTH)

    transform(4, [g_raw[z] for z in range(DEPTH)])
    loads[2].wait()
    pl.semaphore_wait(barrier, OWNERS + RING + GROUPS - 1)

    mine = pl.ds(pl.multiple_of(own * COLS, COLS), COLS)
    here = pl.ds(sp * DEPTH, DEPTH)

    def slab(other, first, size):
        return pl.ds(pl.multiple_of(other * COLS + first, SUB), size)

    for d in range(1, OWNERS):
        other, target = owner(d)
        send(hat.at[4, :, slab(other, 0, COLS), :], gin.at[half, here], GUESS, target)
    send(pair_steps.at[half], pair_steps.at[half], PSTEP, partner)
    gin[half, here] = hat[4, :, mine, :]
    for m in range(4):
        transform(m, [
            step * mixed(QUAD[m], [f_raw[j, z] for j in range(5)]) for z in range(DEPTH)
        ])
        for d in range(1, OWNERS):
            other, target = owner(d)
            send(hat.at[m, :, slab(other, 0, SUB), :], qin.at[0, half, m, here], FIELDS, target)
    for d in range(1, OWNERS):
        other, target = owner(d)
        send(hat.at[pl.ds(0, 4), :, slab(other, SUB, SUB), :], qin.at[1, half, :, here], FIELDS + 1, target)
    for h in range(CHUNKS):
        for m in range(4):
            qin[h, half, m, here] = hat[m, :, slab(own, h * SUB, SUB), :]

    for load in loads[3:]:
        load.wait()
    first_tiles = (SPACES - 1) * DEPTH * COLS // SUB

    @pl.when(pair == 0)
    def _():
        transform(5, [i_raw[z] for z in range(DEPTH)])
        for d in range(1, SPACES):
            other = lax.rem(sp + d, SPACES)
            describe(
                hat.at[5, :, slab(half * SPACES + other, 0, COLS), :], firsts.at[here], FIRST, (tm, other)
            ).start()
        firsts[here] = hat[5, :, mine, :]

    z_matrix = sine(PLANES)
    z_eigen = eigen(PLANES)
    for h in range(CHUNKS):
        for k in range(PLANES):
            lam[h, pl.ds(k * SUB, SUB), :] = lamxy[pl.ds(h * SUB, SUB), :] + float(z_eigen[k])

    arrived(PSTEP)
    for d in range(1, RING):
        send(pair_steps, all_steps.at[slot], STEPS, along_ring(d)[1])
    all_steps[slot] = pair_steps[...]

    def table(i, carry):
        at = pl.ds(pl.multiple_of(i * 2 * SUB, 2 * SUB), 2 * SUB)
        for h in range(CHUNKS):
            for s in range(2):
                mu = pair_steps[s, 0:1, :] * lam[h, at, :]
                rho, square, v, left, a = responses(mu)
                tab[h, s, 0, at, :] = left
                tab[h, s, 1, at, :] = rho
                tab[h, s, 2, at, :] = a
                tab[h, s, 3, at, :] = square
                for n, m in enumerate((1, 3)):
                    w = [float(x) for x in INTERP[m]]
                    tab[h, s, 4 + 2 * n, at, :] = v[m] - w[0] + w[1] * (left - v[2]) + w[2] * (a - v[4])
                    tab[h, s, 5 + 2 * n, at, :] = w[0] + w[1] * rho + w[2] * square
        return carry

    lax.fori_loop(0, ROWS // (2 * SUB), table, 0)

    arrived(GUESS)
    for s in (1, 0):
        for h in range(CHUNKS):
            planes = along_z([gin[s, z, pl.ds(h * SUB, SUB), :] for z in range(PLANES)], z_matrix)
            for k in range(PLANES):
                ghat[s, h, pl.ds(k * SUB, SUB), :] = planes[k]
        if s == 1:
            send(ghat.at[1], shifted, SHIFT, following)

    def pre(h):
        def step_pre(i, carry):
            two = pl.ds(pl.multiple_of(i * 2 * SUB, 2 * SUB), 2 * SUB)
            forced, extra = [], []
            for s in range(2):
                mu = pair_steps[s, 0:1, :] * lam[h, two, :]
                before = shifted[h, two, :] if s == 0 else ghat[0, h, two, :]
                f, v, left, b = sources([qhat[s, m, two, :] for m in range(4)], ghat[s, h, two, :], before, mu)
                alpha[h, s, 0, two, :] = left
                alpha[h, s, 1, two, :] = b
                for n, m in enumerate((1, 3)):
                    w = [float(x) for x in INTERP[m]]
                    alpha[h, s, 2 + n, two, :] = v[m] + w[1] * (left - v[2]) + w[2] * (b - v[4])
                if s == 0:
                    alpha[h, 0, 4, two, :] = f
                    begin = jnp.where(pair == 0, before, 0.0)
                    square, a = tab[h, 0, 3, two, :], tab[h, 0, 2, two, :]
                    f = f + square * begin
                    b = b + (square + a) * begin
                forced.append(f)
                extra.append(b)
            square, a = tab[h, 1, 3, two, :], tab[h, 1, 2, two, :]
            f = square * forced[0] + forced[1]
            b = square * extra[0] + (a * forced[0] + extra[1])
            for n in range(2):
                fb[h, 2 * i + n, 0] = f[n * SUB : (n + 1) * SUB]
                fb[h, 2 * i + n, 1] = b[n * SUB : (n + 1) * SUB]
            return carry

        lax.fori_loop(0, ROWS // (2 * SUB), step_pre, 0)

    for h in range(CHUNKS):
        arrived(FIELDS + h)
        for s in range(2):
            for m in range(4):
                planes = along_z([qin[h, s, m, z] for z in range(PLANES)], z_matrix)
                for k in range(PLANES):
                    qhat[s, m, pl.ds(k * SUB, SUB), :] = planes[k]
        if h == 0:
            arrived(SHIFT)

            @pl.when(pair == 0)
            def _():
                settle(recv_sem.at[FIRST], first_tiles)
                for n in range(CHUNKS):
                    planes = along_z([firsts[z, pl.ds(n * SUB, SUB), :] for z in range(PLANES)], z_matrix)
                    for k in range(PLANES):
                        shifted[n, pl.ds(k * SUB, SUB), :] = planes[k]

        pre(h)
        for d in range(1, RING):
            other, target = along_ring(d)
            send(fb.at[h, other], scan_in.at[h, slot], SCAN + h, target)
        scan_in[h, slot] = fb[h, slot]

    arrived(STEPS)
    share = pl.ds(pl.multiple_of(slot * SUB, SUB), SUB)

    def pair_gain(i, carry):
        out = []
        for h in range(CHUNKS):
            total_g, total_a = carry[h]
            gains[i, 2, h] = total_g
            gains[i, 3, h] = total_a
            _, g0, _, _, a0 = responses(all_steps[i, 0, 0:1, :] * lam[h, share, :])
            _, g1, _, _, a1 = responses(all_steps[i, 1, 0:1, :] * lam[h, share, :])
            g, a = g1 * g0, g1 * a0 + a1 * g0
            gains[i, 0, h] = g
            gains[i, 1, h] = a
            out.append((g * total_g, g * total_a + a * total_g))
        return tuple(out)

    ones = jnp.ones((SUB, WIDTH), jnp.float32)
    zero = jnp.zeros((SUB, WIDTH), jnp.float32)
    ends = lax.fori_loop(0, RING, pair_gain, ((ones, zero),) * CHUNKS)
    for h in range(CHUNKS):
        gain_all[group, 0, h] = ends[h][0]
        gain_all[group, 1, h] = ends[h][1]
    for d in range(1, GROUPS):
        send(gain_all.at[group], gain_all.at[group], GAINS, across(d))

    for h in range(CHUNKS):
        arrived(SCAN + h)
        c, d = zero, zero
        for i in range(RING):
            f, b = scan_in[h, i, 0], scan_in[h, i, 1]
            back[h, i, 0] = c
            back[h, i, 1] = d
            g, a = gains[i, 0, h], gains[i, 1, h]
            c, d = g * c + f, g * d + (a * c + b)
        totals[h, group, 0] = c
        totals[h, group, 1] = d
        for n in range(1, GROUPS):
            send(totals.at[h, group], totals.at[h, group], TOTALS + h, across(n))
    arrived(GAINS)
    for h in range(CHUNKS):
        arrived(TOTALS + h)
        c, d = zero, zero
        start_c, start_d = zero, zero
        for other in range(GROUPS - 1):
            g, a = gain_all[other, 0, h], gain_all[other, 1, h]
            c, d = g * c + totals[h, other, 0], g * d + (a * c + totals[h, other, 1])
            start_c = jnp.where(group == other + 1, c, start_c)
            start_d = jnp.where(group == other + 1, d, start_d)
        for i in range(RING):
            g, a = gains[i, 2, h], gains[i, 3, h]
            back[h, i, 0] = back[h, i, 0] + g * start_c
            back[h, i, 1] = back[h, i, 1] + (g * start_d + a * start_c)
        for n in range(1, RING):
            other, target = along_ring(n)
            send(back.at[h, other], cd.at[h, slot], BACK + h, target)
        cd[h, slot] = back[h, slot]

    order = (0, 4, 2, 1, 3)
    for h in range(CHUNKS):
        arrived(BACK + h)
        for k in range(PLANES):
            at = pl.ds(k * SUB, SUB)
            before = shifted[h, at, :]
            c = jnp.where(pair == 0, before, cd[h, k, 0])
            d = jnp.where(pair == 0, before, cd[h, k, 1])
            g, a = tab[h, 0, 3, at, :], tab[h, 0, 2, at, :]
            cd[h, k, 0] = c
            cd[h, k, 1] = d
            cd_odd[h, k, 0] = g * c + alpha[h, 0, 4, at, :]
            cd_odd[h, k, 1] = g * d + (a * c + alpha[h, 0, 1, at, :])
        for m in order:
            rows = []
            for s in range(2):
                src = cd if s == 0 else cd_odd
                planes = []
                for k in range(PLANES):
                    at = pl.ds(k * SUB, SUB)
                    if m == 0:
                        planes.append(src[h, k, 1])
                    else:
                        n = {2: 0, 4: 1, 1: 2, 3: 3}[m]
                        planes.append(
                            alpha[h, s, n, at, :]
                            + (tab[h, s, 2 * n, at, :] * src[h, k, 0] + tab[h, s, 2 * n + 1, at, :] * src[h, k, 1])
                        )
                rows += along_z(planes, z_matrix)
            rows = product(halves(jnp.concatenate(rows, axis=0)), matrix())
            yout[h, m] = rows.reshape(2, PLANES, SUB, WIDTH)
            if h == CHUNKS - 1:
                for d in range(1, OWNERS):
                    other, target = owner(d)
                    send(
                        yout.at[h, m, other // SPACES, pl.ds(lax.rem(other, SPACES) * DEPTH, DEPTH)],
                        outr.at[m, :, slab(own, h * SUB, SUB), :], LAST + m, target,
                    )
            outr[m, :, slab(own, h * SUB, SUB), :] = yout[h, m, half, here]
        if h < CHUNKS - 1:
            for d in range(1, OWNERS):
                other, target = owner(d)
                send(
                    yout.at[h, :, other // SPACES, pl.ds(lax.rem(other, SPACES) * DEPTH, DEPTH)],
                    outr.at[:, :, slab(own, h * SUB, SUB), :], OUT, target,
                )

    arrived(OUT)
    for m in order:
        arrived(LAST + m)
        wide = jnp.concatenate([outr[m, z] for z in range(DEPTH)], axis=1)
        wide = product(matrix(), halves(wide))
        for z in range(DEPTH):
            out_ref[0, m, z] = wide[:, z * WIDTH : (z + 1) * WIDTH]

    for phase, count in sent.items():
        settle(send_sem.at[phase], count)

    @pl.when(pair == 0)
    def _():
        settle(send_sem.at[FIRST], first_tiles)


def body(initial, start_guess, forcing, step_size):
    table = jnp.asarray(sine(WIDTH), jnp.float32)
    lamxy = jnp.asarray(eigen(WIDTH)[:, None] + eigen(WIDTH)[None, :], jnp.float32)
    hbm = pl.BlockSpec(memory_space=pltpu.HBM)
    f32 = lambda *shape: pltpu.VMEM(shape, jnp.float32)
    dma = lambda *shape: pltpu.SemaphoreType.DMA(shape)
    tile = (SUB, WIDTH)
    bf16 = pltpu.VMEM((WIDTH, WIDTH), jnp.bfloat16)
    start_guess, forcing, initial, table, lamxy = (
        pltpu.with_memory_space_constraint(x, pltpu.HBM)
        for x in (start_guess, forcing, initial, table, lamxy)
    )
    return pl.pallas_call(
        kernel,
        out_shape=jax.ShapeDtypeStruct((1, 5, DEPTH, WIDTH, WIDTH), jnp.float32),
        in_specs=[hbm, hbm, hbm, pl.BlockSpec(memory_space=pltpu.SMEM), hbm, hbm],
        out_specs=pl.BlockSpec(memory_space=pltpu.VMEM),
        scratch_shapes=[
            f32(5, DEPTH, WIDTH, WIDTH), f32(DEPTH, WIDTH, WIDTH), f32(DEPTH, WIDTH, WIDTH),
            f32(WIDTH, WIDTH), f32(COLS, WIDTH), bf16, bf16,
            f32(6, DEPTH, WIDTH, WIDTH),
            f32(2, PLANES, COLS, WIDTH), f32(CHUNKS, 2, 4, PLANES, *tile), f32(PLANES, COLS, WIDTH),
            f32(2, CHUNKS, ROWS, WIDTH), f32(2, 4, ROWS, WIDTH), f32(CHUNKS, ROWS, WIDTH),
            f32(CHUNKS, ROWS, WIDTH), f32(CHUNKS, 2, 8, ROWS, WIDTH), f32(CHUNKS, 2, 5, ROWS, WIDTH),
            f32(2, *tile), f32(RING, 2, *tile), f32(RING, 4, CHUNKS, *tile), f32(GROUPS, 2, CHUNKS, *tile),
            f32(CHUNKS, RING, 2, *tile), f32(CHUNKS, RING, 2, *tile), f32(CHUNKS, GROUPS, 2, *tile),
            f32(CHUNKS, RING, 2, *tile), f32(CHUNKS, RING, 2, *tile), f32(CHUNKS, RING, 2, *tile),
            f32(CHUNKS, 5, 2, PLANES, *tile), f32(5, DEPTH, WIDTH, WIDTH), f32(80, *tile),
            dma(5), dma(PHASES), dma(PHASES),
        ],
        compiler_params=pltpu.CompilerParams(
            collective_id=0, has_side_effects=True, vmem_limit_bytes=16 * 1024 * 1024
        ),
    )(start_guess, forcing, initial, step_size, table, lamxy)


def solution(mesh):
    placed = (
        P("space", None, None),
        P("tm", "space", None, None),
        P("tm", None, "space", None, None),
        P("tm"),
    )
    return jax.shard_map(
        body,
        mesh=mesh,
        in_specs=placed,
        out_specs=P("tm", None, "space", None, None),
        check_vma=False,
    )
```

```python
import functools
import math

import jax
import jax.numpy as jnp
import numpy as np
from jax import lax
from jax.experimental import pallas as pl
from jax.experimental.pallas import tpu as pltpu
from jax.sharding import PartitionSpec as P

MESH = pl.DeviceIdType.MESH
GROUPS = 4
RING = 8
PLANES = 8
SPACES = 4
OWNERS = 2 * SPACES
DEPTH = PLANES // SPACES
WIDTH = 128
COLS = WIDTH // OWNERS
SUB = 8
CHUNKS = COLS // SUB
ROWS = PLANES * SUB

OWNER_ORDER = (4, 3, 5, 2, 6, 1, 7)
RING_ORDER = (4, 3, 5, 2, 6, 1, 7)
GROUP_ORDER = (2, 1, 3)

GUESS, FIRST, PSTEP, STEPS, GAINS, OUT, LAST = range(7)
SHIFT, FIELDS, SCAN, TOTALS, BACK = (7 + n * CHUNKS for n in range(5))
PHASES = 7 + 5 * CHUNKS


def node_tables():
    radical = math.sqrt(3.0 / 7.0)
    times = [0.0, (1.0 - radical) / 2.0, 0.5, (1.0 + radical) / 2.0, 1.0]
    integrals = np.zeros((4, 5))
    for column in range(5):
        coeffs = np.array([1.0])
        for other in range(5):
            if other != column:
                coeffs = np.convolve(coeffs, [-times[other], 1.0]) / (times[column] - times[other])
        powers = np.arange(1, 6)
        for section in range(4):
            integrals[section, column] = np.sum(
                coeffs * (times[section + 1] ** powers - times[section] ** powers) / powers
            )
    coarse = [0.0, 0.5, 1.0]
    interp = np.zeros((5, 3))
    for column in range(3):
        for section in range(5):
            weight = 1.0
            for other in range(3):
                if other != column:
                    weight *= (times[section] - coarse[other]) / (coarse[column] - coarse[other])
            interp[section, column] = weight
    return times, integrals, interp


TIMES, QUAD, INTERP = node_tables()
SPACING = [TIMES[m + 1] - TIMES[m] for m in range(4)]


def mixed(weights, values):
    total = None
    for weight, value in zip(weights, values):
        if value is None or abs(weight) < 1e-14:
            continue
        term = float(weight) * value
        total = term if total is None else total + term
    return total


def sweep(u, q, mu):
    v = [u[0]]
    for m in range(4):
        weights = list(QUAD[m])
        weights[m] -= SPACING[m]
        rate = mixed(weights + [SPACING[m]], u + [v[m]])
        new = -mu * rate
        if q is not None:
            new = new + q[m]
        if v[m] is not None:
            new = new + v[m]
        v.append(new)
    return v


def coarse_terms(v, q, mu):
    weights = QUAD[0] + QUAD[1]
    weights[0] -= 0.5
    left = -mu * mixed(weights, v)
    weights = QUAD[2] + QUAD[3]
    weights[2] -= 0.5
    right = -mu * mixed(weights, v)
    if q is not None:
        left = left + (q[0] + q[1])
        right = right + (q[2] + q[3])
    return left, right


def sources(q, guess, before, mu):
    rho = 1.0 - 0.5 * mu
    v = sweep([before, guess, guess, guess, guess], q, mu)
    left, right = coarse_terms(v, q, mu)
    forced = rho * left + right
    u = [None, None, left, None, forced]
    for m in (1, 3):
        u[m] = v[m] + mixed(INTERP[m], [-before, left - v[2], forced - v[4]])
    v = sweep(u, q, mu)
    left2, right2 = coarse_terms(v, q, mu)
    return forced, v, left2, rho * left2 + right2


def responses(mu):
    rho = 1.0 - 0.5 * mu
    square = rho * rho
    u = [1.0, None, rho, None, square]
    for m in (1, 3):
        u[m] = float(INTERP[m, 0]) + float(INTERP[m, 1]) * rho + float(INTERP[m, 2]) * square
    v = sweep(u, None, mu)
    left, right = coarse_terms(v, None, mu)
    return rho, square, v, left, rho * left + right


def sine(length):
    k = np.arange(1, length + 1)
    return math.sqrt(2.0 / (length + 1)) * np.sin(math.pi / (length + 1) * np.outer(k, k))


def eigen(length):
    return 2.0 - 2.0 * np.cos(math.pi / (length + 1) * np.arange(1, length + 1))


def along_z(planes, matrix):
    n = len(planes)
    half = n // 2
    even = [planes[i] + planes[n - 1 - i] for i in range(half)]
    odd = [planes[i] - planes[n - 1 - i] for i in range(half)]
    out = []
    for k in range(n):
        out.append(mixed(matrix[k][:half], even if k % 2 == 0 else odd))
    return out


def kernel(
    start_hbm, force_hbm, first_hbm, step_ref, sin_hbm, lamxy_hbm, out_ref,
    f_raw, g_raw, i_raw, sin_ref, lamxy, sin_hi, sin_lo, hat, gin, qin, firsts, ghat, qhat,
    shifted, lam, tab, alpha, pair_steps, all_steps, gains, gain_all, fb, scan_in, totals, back, cd,
    cd_odd, yout, outr, measure, load_sem, send_sem, recv_sem,
):
    tm = lax.axis_index("tm")
    sp = lax.axis_index("space")
    pair, half = tm // 2, tm % 2
    group, slot = pair // RING, pair % RING
    own = half * SPACES + sp

    def halves(x):
        hi = x.astype(jnp.bfloat16)
        return hi, (x - hi.astype(jnp.float32)).astype(jnp.bfloat16)

    def product(a, b):
        dot = functools.partial(jnp.dot, preferred_element_type=jnp.float32)
        return dot(a[0], b[0]) + (dot(a[0], b[1]) + dot(a[1], b[0]))

    def matrix():
        return sin_hi[...], sin_lo[...]

    def owner(d):
        other = lax.rem(own + d, OWNERS)
        return other, (pair * 2 + other // SPACES, lax.rem(other, SPACES))

    def along_ring(d):
        other = lax.rem(slot + d, RING)
        return other, ((group * RING + other) * 2 + half, sp)

    def across(d):
        return ((lax.rem(group + d, GROUPS) * RING + slot) * 2 + half, sp)

    sent = {}

    def tiles(ref):
        return math.prod(ref.shape) // (SUB * WIDTH)

    def describe(src, dst, phase, target):
        return pltpu.make_async_remote_copy(
            src_ref=src, dst_ref=dst, send_sem=send_sem.at[phase], recv_sem=recv_sem.at[phase],
            device_id=target, device_id_type=MESH,
        )

    def send(src, dst, phase, target):
        describe(src, dst, phase, target).start()
        sent[phase] = sent.get(phase, 0) + tiles(src)

    def settle(sem, count):
        some = measure.at[pl.ds(0, count)]
        pltpu.make_async_copy(some, some, sem).wait()

    def arrived(phase):
        settle(recv_sem.at[phase], sent[phase])

    pairs = GROUPS * RING
    following = (lax.rem(pair + 1, pairs) * 2 + half, sp)
    preceding = (lax.rem(pair + pairs - 1, pairs) * 2 + half, sp)
    partner = (pair * 2 + 1 - half, lax.rem(sp + SPACES // 2, SPACES))

    loads = [
        pltpu.make_async_copy(start_hbm.at[0], g_raw, load_sem.at[0]),
        pltpu.make_async_copy(sin_hbm, sin_ref, load_sem.at[1]),
        pltpu.make_async_copy(force_hbm.at[0], f_raw, load_sem.at[2]),
        pltpu.make_async_copy(lamxy_hbm.at[pl.ds(pl.multiple_of(own * COLS, COLS), COLS)], lamxy, load_sem.at[3]),
        pltpu.make_async_copy(first_hbm, i_raw, load_sem.at[4]),
    ]
    for load in loads:
        load.start()

    barrier = pltpu.get_barrier_semaphore()

    def greet(target):
        pl.semaphore_signal(barrier, inc=1, device_id=target, device_id_type=MESH)

    for d in RING_ORDER:
        greet(along_ring(d)[1])
    for d in GROUP_ORDER:
        greet(across(d))
    for d in OWNER_ORDER:
        greet(owner(d)[1])
    greet(following)
    greet(preceding)

    for load in loads[:2]:
        load.wait()
    step = step_ref[0]
    pair_steps[half] = jnp.full((SUB, WIDTH), step, jnp.float32)
    sin_hi[...], sin_lo[...] = halves(sin_ref[...])

    def transform(f, planes):
        wide = product(matrix(), halves(jnp.concatenate(planes, axis=1)))
        tall = jnp.concatenate([wide[:, z * WIDTH : (z + 1) * WIDTH] for z in range(DEPTH)], axis=0)
        hat[f] = product(halves(tall), matrix()).reshape(DEPTH, WIDTH, WIDTH)

    transform(4, [g_raw[z] for z in range(DEPTH)])
    loads[2].wait()
    pl.semaphore_wait(barrier, OWNERS + RING + GROUPS - 1)

    mine = pl.ds(pl.multiple_of(own * COLS, COLS), COLS)
    here = pl.ds(sp * DEPTH, DEPTH)

    def slab(other, first, size):
        return pl.ds(pl.multiple_of(other * COLS + first, SUB), size)

    send(pair_steps.at[half], pair_steps.at[half], PSTEP, partner)
    for d in OWNER_ORDER:
        other, target = owner(d)
        send(hat.at[4, :, slab(other, 0, COLS), :], gin.at[half, here], GUESS, target)
    gin[half, here] = hat[4, :, mine, :]
    for m in range(4):
        transform(m, [
            step * mixed(QUAD[m], [f_raw[j, z] for j in range(5)]) for z in range(DEPTH)
        ])
        for d in OWNER_ORDER:
            other, target = owner(d)
            send(hat.at[m, :, slab(other, 0, SUB), :], qin.at[0, half, m, here], FIELDS, target)
    for h in range(CHUNKS):
        for m in range(4):
            qin[h, half, m, here] = hat[m, :, slab(own, h * SUB, SUB), :]

    for load in loads[3:]:
        load.wait()
    first_tiles = (SPACES - 1) * DEPTH * COLS // SUB

    @pl.when(pair == 0)
    def _():
        transform(5, [i_raw[z] for z in range(DEPTH)])
        for d in range(1, SPACES):
            other = lax.rem(sp + d, SPACES)
            describe(
                hat.at[5, :, slab(half * SPACES + other, 0, COLS), :], firsts.at[here], FIRST, (tm, other)
            ).start()
        firsts[here] = hat[5, :, mine, :]

    z_matrix = sine(PLANES)
    z_eigen = eigen(PLANES)
    for h in range(CHUNKS):
        for k in range(PLANES):
            lam[h, pl.ds(k * SUB, SUB), :] = lamxy[pl.ds(h * SUB, SUB), :] + float(z_eigen[k])

    arrived(PSTEP)
    for d in RING_ORDER:
        send(pair_steps, all_steps.at[slot], STEPS, along_ring(d)[1])
    all_steps[slot] = pair_steps[...]

    def table(i, carry):
        at = pl.ds(pl.multiple_of(i * 2 * SUB, 2 * SUB), 2 * SUB)
        for h in range(CHUNKS):
            for s in range(2):
                mu = pair_steps[s, 0:1, :] * lam[h, at, :]
                rho, square, v, left, a = responses(mu)
                tab[h, s, 0, at, :] = left
                tab[h, s, 1, at, :] = rho
                tab[h, s, 2, at, :] = a
                tab[h, s, 3, at, :] = square
                for n, m in enumerate((1, 3)):
                    w = [float(x) for x in INTERP[m]]
                    tab[h, s, 4 + 2 * n, at, :] = v[m] - w[0] + w[1] * (left - v[2]) + w[2] * (a - v[4])
                    tab[h, s, 5 + 2 * n, at, :] = w[0] + w[1] * rho + w[2] * square
        return carry

    lax.fori_loop(0, ROWS // (2 * SUB), table, 0)

    arrived(GUESS)
    for s in (1, 0):
        for h in range(CHUNKS):
            planes = along_z([gin[s, z, pl.ds(h * SUB, SUB), :] for z in range(PLANES)], z_matrix)
            for k in range(PLANES):
                ghat[s, h, pl.ds(k * SUB, SUB), :] = planes[k]
            if s == 1:
                send(ghat.at[1, h], shifted.at[h], SHIFT + h, following)

    for d in OWNER_ORDER:
        other, target = owner(d)
        send(hat.at[pl.ds(0, 4), :, slab(other, SUB, SUB), :], qin.at[1, half, :, here], FIELDS + 1, target)

    def pre(h):
        def step_pre(i, carry):
            two = pl.ds(pl.multiple_of(i * 2 * SUB, 2 * SUB), 2 * SUB)
            forced, extra = [], []
            for s in range(2):
                mu = pair_steps[s, 0:1, :] * lam[h, two, :]
                before = shifted[h, two, :] if s == 0 else ghat[0, h, two, :]
                f, v, left, b = sources([qhat[s, m, two, :] for m in range(4)], ghat[s, h, two, :], before, mu)
                alpha[h, s, 0, two, :] = left
                alpha[h, s, 1, two, :] = b
                for n, m in enumerate((1, 3)):
                    w = [float(x) for x in INTERP[m]]
                    alpha[h, s, 2 + n, two, :] = v[m] + w[1] * (left - v[2]) + w[2] * (b - v[4])
                if s == 0:
                    alpha[h, 0, 4, two, :] = f
                    begin = jnp.where(pair == 0, before, 0.0)
                    square, a = tab[h, 0, 3, two, :], tab[h, 0, 2, two, :]
                    f = f + square * begin
                    b = b + (square + a) * begin
                forced.append(f)
                extra.append(b)
            square, a = tab[h, 1, 3, two, :], tab[h, 1, 2, two, :]
            f = square * forced[0] + forced[1]
            b = square * extra[0] + (a * forced[0] + extra[1])
            for n in range(2):
                fb[h, 2 * i + n, 0] = f[n * SUB : (n + 1) * SUB]
                fb[h, 2 * i + n, 1] = b[n * SUB : (n + 1) * SUB]
            return carry

        lax.fori_loop(0, ROWS // (2 * SUB), step_pre, 0)

    for h in range(CHUNKS):
        arrived(FIELDS + h)
        for s in range(2):
            for m in range(4):
                planes = along_z([qin[h, s, m, z] for z in range(PLANES)], z_matrix)
                for k in range(PLANES):
                    qhat[s, m, pl.ds(k * SUB, SUB), :] = planes[k]
        arrived(SHIFT + h)

        @pl.when(pair == 0)
        def _():
            if h == 0:
                settle(recv_sem.at[FIRST], first_tiles)
            planes = along_z([firsts[z, pl.ds(h * SUB, SUB), :] for z in range(PLANES)], z_matrix)
            for k in range(PLANES):
                shifted[h, pl.ds(k * SUB, SUB), :] = planes[k]

        pre(h)
        for d in RING_ORDER:
            other, target = along_ring(d)
            send(fb.at[h, other], scan_in.at[h, slot], SCAN + h, target)
        scan_in[h, slot] = fb[h, slot]

    arrived(STEPS)
    share = pl.ds(pl.multiple_of(slot * SUB, SUB), SUB)

    def pair_gain(i, carry):
        out = []
        for h in range(CHUNKS):
            total_g, total_a = carry[h]
            gains[i, 2, h] = total_g
            gains[i, 3, h] = total_a
            _, g0, _, _, a0 = responses(all_steps[i, 0, 0:1, :] * lam[h, share, :])
            _, g1, _, _, a1 = responses(all_steps[i, 1, 0:1, :] * lam[h, share, :])
            g, a = g1 * g0, g1 * a0 + a1 * g0
            gains[i, 0, h] = g
            gains[i, 1, h] = a
            out.append((g * total_g, g * total_a + a * total_g))
        return tuple(out)

    ones = jnp.ones((SUB, WIDTH), jnp.float32)
    zero = jnp.zeros((SUB, WIDTH), jnp.float32)
    ends = lax.fori_loop(0, RING, pair_gain, ((ones, zero),) * CHUNKS)
    for h in range(CHUNKS):
        gain_all[group, 0, h] = ends[h][0]
        gain_all[group, 1, h] = ends[h][1]
    for d in GROUP_ORDER:
        send(gain_all.at[group], gain_all.at[group], GAINS, across(d))

    for h in range(CHUNKS):
        arrived(SCAN + h)
        c, d = zero, zero
        for i in range(RING):
            f, b = scan_in[h, i, 0], scan_in[h, i, 1]
            back[h, i, 0] = c
            back[h, i, 1] = d
            g, a = gains[i, 0, h], gains[i, 1, h]
            c, d = g * c + f, g * d + (a * c + b)
        totals[h, group, 0] = c
        totals[h, group, 1] = d
        for n in GROUP_ORDER:
            send(totals.at[h, group], totals.at[h, group], TOTALS + h, across(n))
    arrived(GAINS)
    for h in range(CHUNKS):
        arrived(TOTALS + h)
        c, d = zero, zero
        start_c, start_d = zero, zero
        for other in range(GROUPS - 1):
            g, a = gain_all[other, 0, h], gain_all[other, 1, h]
            c, d = g * c + totals[h, other, 0], g * d + (a * c + totals[h, other, 1])
            start_c = jnp.where(group == other + 1, c, start_c)
            start_d = jnp.where(group == other + 1, d, start_d)
        for i in range(RING):
            g, a = gains[i, 2, h], gains[i, 3, h]
            back[h, i, 0] = back[h, i, 0] + g * start_c
            back[h, i, 1] = back[h, i, 1] + (g * start_d + a * start_c)
        for n in RING_ORDER:
            other, target = along_ring(n)
            send(back.at[h, other], cd.at[h, slot], BACK + h, target)
        cd[h, slot] = back[h, slot]

    for h in range(CHUNKS):
        arrived(BACK + h)
        for k in range(PLANES):
            at = pl.ds(k * SUB, SUB)
            before = shifted[h, at, :]
            c = jnp.where(pair == 0, before, cd[h, k, 0])
            d = jnp.where(pair == 0, before, cd[h, k, 1])
            g, a = tab[h, 0, 3, at, :], tab[h, 0, 2, at, :]
            cd[h, k, 0] = c
            cd[h, k, 1] = d
            cd_odd[h, k, 0] = g * c + alpha[h, 0, 4, at, :]
            cd_odd[h, k, 1] = g * d + (a * c + alpha[h, 0, 1, at, :])
        rows = []
        for m in range(5):
            for s in range(2):
                src = cd if s == 0 else cd_odd
                planes = []
                for k in range(PLANES):
                    at = pl.ds(k * SUB, SUB)
                    if m == 0:
                        planes.append(src[h, k, 1])
                    else:
                        n = {2: 0, 4: 1, 1: 2, 3: 3}[m]
                        planes.append(
                            alpha[h, s, n, at, :]
                            + (tab[h, s, 2 * n, at, :] * src[h, k, 0] + tab[h, s, 2 * n + 1, at, :] * src[h, k, 1])
                        )
                rows += along_z(planes, z_matrix)
        rows = product(halves(jnp.concatenate(rows, axis=0)), matrix())
        yout[h] = rows.reshape(5, 2, PLANES, SUB, WIDTH)
        for d in OWNER_ORDER:
            other, target = owner(d)
            send(
                yout.at[h, :, other // SPACES, pl.ds(lax.rem(other, SPACES) * DEPTH, DEPTH)],
                outr.at[:, :, slab(own, h * SUB, SUB), :], OUT if h < CHUNKS - 1 else LAST, target,
            )
        outr[:, :, slab(own, h * SUB, SUB), :] = yout[h, :, half, here]

    arrived(OUT)
    arrived(LAST)
    for m in range(5):
        wide = jnp.concatenate([outr[m, z] for z in range(DEPTH)], axis=1)
        wide = product(matrix(), halves(wide))
        for z in range(DEPTH):
            out_ref[0, m, z] = wide[:, z * WIDTH : (z + 1) * WIDTH]

    for phase, count in sent.items():
        settle(send_sem.at[phase], count)

    @pl.when(pair == 0)
    def _():
        settle(send_sem.at[FIRST], first_tiles)


def body(initial, start_guess, forcing, step_size):
    table = jnp.asarray(sine(WIDTH), jnp.float32)
    lamxy = jnp.asarray(eigen(WIDTH)[:, None] + eigen(WIDTH)[None, :], jnp.float32)
    hbm = pl.BlockSpec(memory_space=pltpu.HBM)
    f32 = lambda *shape: pltpu.VMEM(shape, jnp.float32)
    dma = lambda *shape: pltpu.SemaphoreType.DMA(shape)
    tile = (SUB, WIDTH)
    bf16 = pltpu.VMEM((WIDTH, WIDTH), jnp.bfloat16)
    start_guess, forcing, initial, table, lamxy = (
        pltpu.with_memory_space_constraint(x, pltpu.HBM)
        for x in (start_guess, forcing, initial, table, lamxy)
    )
    return pl.pallas_call(
        kernel,
        out_shape=jax.ShapeDtypeStruct((1, 5, DEPTH, WIDTH, WIDTH), jnp.float32),
        in_specs=[hbm, hbm, hbm, pl.BlockSpec(memory_space=pltpu.SMEM), hbm, hbm],
        out_specs=pl.BlockSpec(memory_space=pltpu.VMEM),
        scratch_shapes=[
            f32(5, DEPTH, WIDTH, WIDTH), f32(DEPTH, WIDTH, WIDTH), f32(DEPTH, WIDTH, WIDTH),
            f32(WIDTH, WIDTH), f32(COLS, WIDTH), bf16, bf16,
            f32(6, DEPTH, WIDTH, WIDTH),
            f32(2, PLANES, COLS, WIDTH), f32(CHUNKS, 2, 4, PLANES, *tile), f32(PLANES, COLS, WIDTH),
            f32(2, CHUNKS, ROWS, WIDTH), f32(2, 4, ROWS, WIDTH), f32(CHUNKS, ROWS, WIDTH),
            f32(CHUNKS, ROWS, WIDTH), f32(CHUNKS, 2, 8, ROWS, WIDTH), f32(CHUNKS, 2, 5, ROWS, WIDTH),
            f32(2, *tile), f32(RING, 2, *tile), f32(RING, 4, CHUNKS, *tile), f32(GROUPS, 2, CHUNKS, *tile),
            f32(CHUNKS, RING, 2, *tile), f32(CHUNKS, RING, 2, *tile), f32(CHUNKS, GROUPS, 2, *tile),
            f32(CHUNKS, RING, 2, *tile), f32(CHUNKS, RING, 2, *tile), f32(CHUNKS, RING, 2, *tile),
            f32(CHUNKS, 5, 2, PLANES, *tile), f32(5, DEPTH, WIDTH, WIDTH), f32(80, *tile),
            dma(5), dma(PHASES), dma(PHASES),
        ],
        compiler_params=pltpu.CompilerParams(
            collective_id=0, has_side_effects=True, vmem_limit_bytes=16 * 1024 * 1024
        ),
    )(start_guess, forcing, initial, step_size, table, lamxy)


def solution(mesh):
    placed = (
        P("space", None, None),
        P("tm", "space", None, None),
        P("tm", None, "space", None, None),
        P("tm"),
    )
    return jax.shard_map(
        body,
        mesh=mesh,
        in_specs=placed,
        out_specs=P("tm", None, "space", None, None),
        check_vma=False,
    )
```

```python
import functools
import math

import jax
import jax.numpy as jnp
import numpy as np
from jax import lax
from jax.experimental import pallas as pl
from jax.experimental.pallas import tpu as pltpu
from jax.sharding import PartitionSpec as P

MESH = pl.DeviceIdType.MESH
GROUPS = 4
RING = 8
PLANES = 8
SPACES = 4
OWNERS = 2 * SPACES
DEPTH = PLANES // SPACES
WIDTH = 128
COLS = WIDTH // OWNERS
SUB = 8
SPLIT = SUB // 2
CHUNKS = COLS // SPLIT

OWNER_ORDER = (4, 3, 5, 2, 6, 1, 7)
RING_ORDER = (4, 3, 5, 2, 6, 1, 7)
GROUP_ORDER = (2, 1, 3)

GUESS, FIRST, PSTEP, STEPS, GAINS, SHIFT = range(6)
FIELDS, SCAN, TOTALS, BACK, OUT = (8 + n * CHUNKS for n in range(5))
PHASES = 8 + 5 * CHUNKS


def node_tables():
    radical = math.sqrt(3.0 / 7.0)
    times = [0.0, (1.0 - radical) / 2.0, 0.5, (1.0 + radical) / 2.0, 1.0]
    integrals = np.zeros((4, 5))
    for column in range(5):
        coeffs = np.array([1.0])
        for other in range(5):
            if other != column:
                coeffs = np.convolve(coeffs, [-times[other], 1.0]) / (times[column] - times[other])
        powers = np.arange(1, 6)
        for section in range(4):
            integrals[section, column] = np.sum(
                coeffs * (times[section + 1] ** powers - times[section] ** powers) / powers
            )
    coarse = [0.0, 0.5, 1.0]
    interp = np.zeros((5, 3))
    for column in range(3):
        for section in range(5):
            weight = 1.0
            for other in range(3):
                if other != column:
                    weight *= (times[section] - coarse[other]) / (coarse[column] - coarse[other])
            interp[section, column] = weight
    return times, integrals, interp


TIMES, QUAD, INTERP = node_tables()
SPACING = [TIMES[m + 1] - TIMES[m] for m in range(4)]


def mixed(weights, values):
    total = None
    for weight, value in zip(weights, values):
        if value is None or abs(weight) < 1e-14:
            continue
        term = float(weight) * value
        total = term if total is None else total + term
    return total


def sweep(u, q, mu):
    v = [u[0]]
    for m in range(4):
        weights = list(QUAD[m])
        weights[m] -= SPACING[m]
        rate = mixed(weights + [SPACING[m]], u + [v[m]])
        new = -mu * rate
        if q is not None:
            new = new + q[m]
        if v[m] is not None:
            new = new + v[m]
        v.append(new)
    return v


def coarse_terms(v, q, mu):
    weights = QUAD[0] + QUAD[1]
    weights[0] -= 0.5
    left = -mu * mixed(weights, v)
    weights = QUAD[2] + QUAD[3]
    weights[2] -= 0.5
    right = -mu * mixed(weights, v)
    if q is not None:
        left = left + (q[0] + q[1])
        right = right + (q[2] + q[3])
    return left, right


def sources(q, guess, before, mu):
    rho = 1.0 - 0.5 * mu
    v = sweep([before, guess, guess, guess, guess], q, mu)
    left, right = coarse_terms(v, q, mu)
    forced = rho * left + right
    u = [None, None, left, None, forced]
    for m in (1, 3):
        u[m] = v[m] + mixed(INTERP[m], [-before, left - v[2], forced - v[4]])
    v = sweep(u, q, mu)
    left2, right2 = coarse_terms(v, q, mu)
    return forced, v, left2, rho * left2 + right2


def responses(mu):
    rho = 1.0 - 0.5 * mu
    square = rho * rho
    u = [1.0, None, rho, None, square]
    for m in (1, 3):
        u[m] = float(INTERP[m, 0]) + float(INTERP[m, 1]) * rho + float(INTERP[m, 2]) * square
    v = sweep(u, None, mu)
    left, right = coarse_terms(v, None, mu)
    return rho, square, v, left, rho * left + right


def sine(length):
    k = np.arange(1, length + 1)
    return math.sqrt(2.0 / (length + 1)) * np.sin(math.pi / (length + 1) * np.outer(k, k))


def eigen(length):
    return 2.0 - 2.0 * np.cos(math.pi / (length + 1) * np.arange(1, length + 1))


def along_z(planes, matrix):
    n = len(planes)
    half = n // 2
    even = [planes[i] + planes[n - 1 - i] for i in range(half)]
    odd = [planes[i] - planes[n - 1 - i] for i in range(half)]
    out = []
    for k in range(n):
        out.append(mixed(matrix[k][:half], even if k % 2 == 0 else odd))
    return out


def kernel(
    start_hbm, force_hbm, first_hbm, step_ref, sin_hbm, lamxy_hbm, out_ref,
    f_raw, g_raw, i_raw, sin_ref, lamxy, sin_hi, sin_lo, hat, gin, qin, firsts, ghat, shifted, guess,
    earlier, qhat, lam, tab, alpha, pair_steps, step_tile, all_steps, gains, gain_all, fb, scan_in,
    totals, partial, back, cd, starts, yout, outr, measure, load_sem, send_sem, recv_sem, local_sem,
):
    tm = lax.axis_index("tm")
    sp = lax.axis_index("space")
    pair, half = tm // 2, tm % 2
    group, slot = pair // RING, pair % RING
    own = half * SPACES + sp

    def halves(x):
        hi = x.astype(jnp.bfloat16)
        return hi, (x - hi.astype(jnp.float32)).astype(jnp.bfloat16)

    def product(a, b):
        dot = functools.partial(jnp.dot, preferred_element_type=jnp.float32)
        return dot(a[0], b[0]) + (dot(a[0], b[1]) + dot(a[1], b[0]))

    def matrix():
        return sin_hi[...], sin_lo[...]

    def owner(d):
        other = lax.rem(own + d, OWNERS)
        return other, (pair * 2 + other // SPACES, lax.rem(other, SPACES))

    def along_ring(d):
        other = lax.rem(slot + d, RING)
        return other, ((group * RING + other) * 2 + half, sp)

    def across(d):
        return ((lax.rem(group + d, GROUPS) * RING + slot) * 2 + half, sp)

    sent = {}

    def describe(src, dst, phase, target):
        return pltpu.make_async_remote_copy(
            src_ref=src, dst_ref=dst, send_sem=send_sem.at[phase], recv_sem=recv_sem.at[phase],
            device_id=target, device_id_type=MESH,
        )

    def send(src, dst, phase, target):
        describe(src, dst, phase, target).start()
        sent[phase] = sent.get(phase, 0) + math.prod(src.shape)

    def settle(sem, count):
        some = measure.at[pl.ds(0, count // (SUB * WIDTH))]
        pltpu.make_async_copy(some, some, sem).wait()

    def arrived(phase):
        settle(recv_sem.at[phase], sent[phase])

    pairs = GROUPS * RING
    following = (lax.rem(pair + 1, pairs) * 2 + half, sp)
    preceding = (lax.rem(pair + pairs - 1, pairs) * 2 + half, sp)
    partner = (pair * 2 + 1 - half, lax.rem(sp + SPACES // 2, SPACES))

    loads = [
        pltpu.make_async_copy(start_hbm.at[0], g_raw, load_sem.at[0]),
        pltpu.make_async_copy(sin_hbm, sin_ref, load_sem.at[1]),
        pltpu.make_async_copy(force_hbm.at[0], f_raw, load_sem.at[2]),
        pltpu.make_async_copy(lamxy_hbm.at[pl.ds(pl.multiple_of(own * COLS, COLS), COLS)], lamxy, load_sem.at[3]),
        pltpu.make_async_copy(first_hbm, i_raw, load_sem.at[4]),
    ]
    for load in loads:
        load.start()

    barrier = pltpu.get_barrier_semaphore()

    def greet(target):
        pl.semaphore_signal(barrier, inc=1, device_id=target, device_id_type=MESH)

    for d in RING_ORDER:
        greet(along_ring(d)[1])
    for d in GROUP_ORDER:
        greet(across(d))
    for d in OWNER_ORDER:
        greet(owner(d)[1])
    greet(following)
    greet(preceding)

    for load in loads[:2]:
        load.wait()
    step = step_ref[0]
    pair_steps[half] = jnp.full((SUB, WIDTH), step, jnp.float32)
    sin_hi[...], sin_lo[...] = halves(sin_ref[...])

    def transform(f, planes):
        wide = product(matrix(), halves(jnp.concatenate(planes, axis=1)))
        tall = jnp.concatenate([wide[:, z * WIDTH : (z + 1) * WIDTH] for z in range(DEPTH)], axis=0)
        hat[f] = product(halves(tall), matrix()).reshape(DEPTH, WIDTH, WIDTH)

    transform(4, [g_raw[z] for z in range(DEPTH)])
    loads[2].wait()
    pl.semaphore_wait(barrier, OWNERS + RING + GROUPS - 1)

    mine = pl.ds(pl.multiple_of(own * COLS, COLS), COLS)
    here = pl.ds(sp * DEPTH, DEPTH)
    part = pl.ds(pl.multiple_of(half * SPLIT, SPLIT), SPLIT)

    def slab(other, first, size):
        return pl.ds(pl.multiple_of(other * COLS + first, SPLIT), size)

    def swap(x):
        return pltpu.roll(x, SPLIT, x.ndim - 2)

    def pick(upper, lower):
        row = lax.broadcasted_iota(jnp.int32, (SUB, WIDTH), 0)
        return jnp.where(row < SPLIT, upper, lower)

    send(pair_steps.at[half], pair_steps.at[half], PSTEP, partner)
    for d in OWNER_ORDER:
        other, target = owner(d)
        send(hat.at[4, :, slab(other, 0, COLS), :], gin.at[half, here], GUESS, target)
    gin[half, here] = hat[4, :, mine, :]
    for m in range(4):
        transform(m, [
            step * mixed(QUAD[m], [f_raw[j, z] for j in range(5)]) for z in range(DEPTH)
        ])
        for d in OWNER_ORDER:
            other, target = owner(d)
            send(hat.at[m, :, slab(other, 0, SPLIT), :], qin.at[0, m, here, part, :], FIELDS, target)
    kept = [
        pltpu.make_async_copy(
            hat.at[pl.ds(0, 4), :, slab(own, h * SPLIT, SPLIT), :], qin.at[h, :, here, part, :], local_sem.at[h]
        )
        for h in range(CHUNKS)
    ]
    for copy in kept:
        copy.start()

    for load in loads[3:]:
        load.wait()
    first_size = (SPACES - 1) * DEPTH * COLS * WIDTH

    @pl.when(pair == 0)
    def _():
        transform(5, [i_raw[z] for z in range(DEPTH)])
        for d in range(1, SPACES):
            other = lax.rem(sp + d, SPACES)
            describe(
                hat.at[5, :, slab(half * SPACES + other, 0, COLS), :], firsts.at[here], FIRST, (tm, other)
            ).start()
        firsts[here] = hat[5, :, mine, :]

    def send_fields(h):
        for d in OWNER_ORDER:
            other, target = owner(d)
            send(
                hat.at[pl.ds(0, 4), :, slab(other, h * SPLIT, SPLIT), :], qin.at[h, :, here, part, :],
                FIELDS + h, target,
            )

    z_matrix = sine(PLANES)
    z_eigen = eigen(PLANES)
    for h in range(CHUNKS):
        both = lamxy[pl.ds(h // 2 * SUB, SUB), :]
        both = pick(both, swap(both)) if h % 2 == 0 else pick(swap(both), both)
        for k in range(PLANES):
            lam[h, k] = both + float(z_eigen[k])

    arrived(PSTEP)
    step_tile[...] = pick(pair_steps[0], pair_steps[1])
    for d in RING_ORDER:
        send(step_tile, all_steps.at[slot], STEPS, along_ring(d)[1])
    all_steps[slot] = step_tile[...]

    def table(i, carry):
        two = pl.ds(i * 2, 2)
        for h in range(CHUNKS):
            mu = step_tile[...] * lam[h, two]
            rho, square, v, left, a = responses(mu)
            tab[h, 0, two] = left
            tab[h, 1, two] = rho
            tab[h, 2, two] = a
            tab[h, 3, two] = square
            for n, m in enumerate((1, 3)):
                w = [float(x) for x in INTERP[m]]
                tab[h, 4 + 2 * n, two] = v[m] - w[0] + w[1] * (left - v[2]) + w[2] * (a - v[4])
                tab[h, 5 + 2 * n, two] = w[0] + w[1] * rho + w[2] * square
            tab[h, 8, two] = pick(1.0, swap(square))
            tab[h, 9, two] = pick(0.0, swap(a))
        return carry

    lax.fori_loop(0, PLANES // 2, table, 0)
    send_fields(1)

    arrived(GUESS)
    for s in (1, 0):
        for n in range(COLS // SUB):
            planes = along_z([gin[s, z, pl.ds(n * SUB, SUB), :] for z in range(PLANES)], z_matrix)
            for k in range(PLANES):
                ghat[s, n, k] = planes[k]
            if s == 1:
                send(ghat.at[1, n], shifted.at[n], SHIFT + n, following)
    for h in range(2, CHUNKS):
        send_fields(h)
    for h in range(CHUNKS):
        for k in range(PLANES):
            upper, lower = ghat[0, h // 2, k], ghat[1, h // 2, k]
            guess[h, k] = pick(upper, swap(lower)) if h % 2 == 0 else pick(swap(upper), lower)

    opening = pick(jnp.where(pair == 0, 1.0, 0.0), 0.0)

    def pre(h):
        def step_pre(i, carry):
            two = pl.ds(i * 2, 2)
            mu = step_tile[...] * lam[h, two]
            before = earlier[h, two]
            f, v, left, b = sources([qhat[m, two] for m in range(4)], guess[h, two], before, mu)
            alpha[h, 0, two] = left
            alpha[h, 1, two] = b
            for n, m in enumerate((1, 3)):
                w = [float(x) for x in INTERP[m]]
                alpha[h, 2 + n, two] = v[m] + w[1] * (left - v[2]) + w[2] * (b - v[4])
            alpha[h, 4, two] = pick(0.0, swap(f))
            alpha[h, 5, two] = pick(0.0, swap(b))
            begin = before * opening
            square, a = tab[h, 3, two], tab[h, 2, two]
            f = f + square * begin
            b = b + (square + a) * begin
            first_f, first_b = swap(f), swap(b)
            pair_f = square * first_f + f
            pair_b = square * first_b + (a * first_f + b)
            fb[h, two] = pick(swap(pair_f), pair_b)
            return carry

        lax.fori_loop(0, PLANES // 2, step_pre, 0)

    for h in range(CHUNKS):
        kept[h].wait()
        arrived(FIELDS + h)
        for m in range(4):
            planes = along_z([qin[h, m, z] for z in range(PLANES)], z_matrix)
            for k in range(PLANES):
                qhat[m, k] = planes[k]
        if h % 2 == 0:
            n = h // 2
            arrived(SHIFT + n)

            @pl.when(pair == 0)
            def _():
                if h == 0:
                    settle(recv_sem.at[FIRST], first_size)
                planes = along_z([firsts[z, pl.ds(n * SUB, SUB), :] for z in range(PLANES)], z_matrix)
                for k in range(PLANES):
                    shifted[n, k] = planes[k]

            for k in range(PLANES):
                upper, lower = shifted[n, k], ghat[0, n, k]
                earlier[h, k] = pick(upper, swap(lower))
                earlier[h + 1, k] = pick(swap(upper), lower)
        pre(h)
        for d in RING_ORDER:
            other, target = along_ring(d)
            send(fb.at[h, other], scan_in.at[h, slot], SCAN + h, target)
        scan_in[h, slot] = fb[h, slot]

    arrived(STEPS)

    def pair_gain(i, carry):
        out = []
        for h in range(CHUNKS):
            total_g, total_a = carry[h]
            gains[i, 2, h] = total_g
            gains[i, 3, h] = total_a
            _, square, _, _, a = responses(all_steps[i] * lam[h, slot])
            other = swap(square)
            g = square * other
            a = other * a
            a = a + swap(a)
            gains[i, 0, h] = g
            gains[i, 1, h] = a
            out.append((g * total_g, g * total_a + a * total_g))
        return tuple(out)

    ones = jnp.ones((SUB, WIDTH), jnp.float32)
    zero = jnp.zeros((SUB, WIDTH), jnp.float32)
    ends = lax.fori_loop(0, RING, pair_gain, ((ones, zero),) * CHUNKS)
    for h in range(CHUNKS):
        gain_all[group, 0, h] = ends[h][0]
        gain_all[group, 1, h] = ends[h][1]
    for d in GROUP_ORDER:
        send(gain_all.at[group], gain_all.at[group], GAINS, across(d))

    def advance(h):
        arrived(SCAN + h)
        c, d = zero, zero
        for i in range(RING):
            f = scan_in[h, i]
            b = swap(f)
            partial[h, i, 0] = c
            partial[h, i, 1] = d
            g, a = gains[i, 0, h], gains[i, 1, h]
            c, d = g * c + f, g * d + (a * c + b)
        totals[h, group] = pick(c, swap(d))
        for n in GROUP_ORDER:
            send(totals.at[h, group], totals.at[h, group], TOTALS + h, across(n))

    def fold(h):
        if h == 0:
            arrived(GAINS)
        arrived(TOTALS + h)
        c, d = zero, zero
        start_c, start_d = zero, zero
        for other in range(GROUPS - 1):
            g, a = gain_all[other, 0, h], gain_all[other, 1, h]
            f = totals[h, other]
            c, d = g * c + f, g * d + (a * c + swap(f))
            start_c = jnp.where(group == other + 1, c, start_c)
            start_d = jnp.where(group == other + 1, d, start_d)
        for i in range(RING):
            g, a = gains[i, 2, h], gains[i, 3, h]
            c = partial[h, i, 0] + g * start_c
            d = partial[h, i, 1] + (g * start_d + a * start_c)
            back[h, i] = pick(c, swap(d))
        for n in RING_ORDER:
            other, target = along_ring(n)
            send(back.at[h, other], cd.at[h, slot], BACK + h, target)
        cd[h, slot] = back[h, slot]

    returned = []

    def give(h):
        arrived(BACK + h)

        @pl.when(pair == 0)
        def _():
            for k in range(PLANES):
                before = earlier[h, k]
                cd[h, k] = pick(before, swap(before))

        for k in range(PLANES):
            tile = cd[h, k]
            turned = swap(tile)
            c, d = pick(tile, turned), pick(turned, tile)
            starts[0, k] = tab[h, 8, k] * c + alpha[h, 4, k]
            starts[1, k] = tab[h, 8, k] * d + (tab[h, 9, k] * c + alpha[h, 5, k])
        rows = []
        for m in range(5):
            planes = []
            for k in range(PLANES):
                if m == 0:
                    planes.append(starts[1, k])
                else:
                    n = {2: 0, 4: 1, 1: 2, 3: 3}[m]
                    planes.append(
                        alpha[h, n, k] + (tab[h, 2 * n, k] * starts[0, k] + tab[h, 2 * n + 1, k] * starts[1, k])
                    )
            rows += along_z(planes, z_matrix)
        rows = product(halves(jnp.concatenate(rows, axis=0)), matrix())
        yout[h] = rows.reshape(5, PLANES, SUB, WIDTH)
        for d in OWNER_ORDER:
            other, target = owner(d)
            rows = pl.ds(pl.multiple_of(other // SPACES * SPLIT, SPLIT), SPLIT)
            send(
                yout.at[h, :, pl.ds(lax.rem(other, SPACES) * DEPTH, DEPTH), rows, :],
                outr.at[:, :, slab(own, h * SPLIT, SPLIT), :], OUT + h, target,
            )
        copy = pltpu.make_async_copy(
            yout.at[h, :, here, part, :], outr.at[:, :, slab(own, h * SPLIT, SPLIT), :], local_sem.at[CHUNKS + h]
        )
        copy.start()
        returned.append(copy)

    advance(0)
    advance(1)
    advance(2)
    fold(0)
    fold(1)
    advance(3)
    fold(2)
    give(0)
    fold(3)
    give(1)
    give(2)
    give(3)

    for h in range(CHUNKS):
        returned[h].wait()
        arrived(OUT + h)
    for m in range(5):
        wide = jnp.concatenate([outr[m, z] for z in range(DEPTH)], axis=1)
        wide = product(matrix(), halves(wide))
        for z in range(DEPTH):
            out_ref[0, m, z] = wide[:, z * WIDTH : (z + 1) * WIDTH]

    for phase, count in sent.items():
        settle(send_sem.at[phase], count)

    @pl.when(pair == 0)
    def _():
        settle(send_sem.at[FIRST], first_size)


def body(initial, start_guess, forcing, step_size):
    table = jnp.asarray(sine(WIDTH), jnp.float32)
    lamxy = jnp.asarray(eigen(WIDTH)[:, None] + eigen(WIDTH)[None, :], jnp.float32)
    hbm = pl.BlockSpec(memory_space=pltpu.HBM)
    f32 = lambda *shape: pltpu.VMEM(shape, jnp.float32)
    dma = lambda *shape: pltpu.SemaphoreType.DMA(shape)
    tile = (SUB, WIDTH)
    bf16 = pltpu.VMEM((WIDTH, WIDTH), jnp.bfloat16)
    start_guess, forcing, initial, table, lamxy = (
        pltpu.with_memory_space_constraint(x, pltpu.HBM)
        for x in (start_guess, forcing, initial, table, lamxy)
    )
    return pl.pallas_call(
        kernel,
        out_shape=jax.ShapeDtypeStruct((1, 5, DEPTH, WIDTH, WIDTH), jnp.float32),
        in_specs=[hbm, hbm, hbm, pl.BlockSpec(memory_space=pltpu.SMEM), hbm, hbm],
        out_specs=pl.BlockSpec(memory_space=pltpu.VMEM),
        scratch_shapes=[
            f32(5, DEPTH, WIDTH, WIDTH), f32(DEPTH, WIDTH, WIDTH), f32(DEPTH, WIDTH, WIDTH),
            f32(WIDTH, WIDTH), f32(COLS, WIDTH), bf16, bf16, f32(6, DEPTH, WIDTH, WIDTH),
            f32(2, PLANES, COLS, WIDTH), f32(CHUNKS, 4, PLANES, *tile), f32(PLANES, COLS, WIDTH),
            f32(2, COLS // SUB, PLANES, *tile), f32(COLS // SUB, PLANES, *tile), f32(CHUNKS, PLANES, *tile),
            f32(CHUNKS, PLANES, *tile), f32(4, PLANES, *tile), f32(CHUNKS, PLANES, *tile),
            f32(CHUNKS, 10, PLANES, *tile), f32(CHUNKS, 6, PLANES, *tile), f32(2, *tile), f32(*tile),
            f32(RING, *tile), f32(RING, 4, CHUNKS, *tile), f32(GROUPS, 2, CHUNKS, *tile),
            f32(CHUNKS, RING, *tile), f32(CHUNKS, RING, *tile), f32(CHUNKS, GROUPS, *tile),
            f32(CHUNKS, RING, 2, *tile), f32(CHUNKS, RING, *tile), f32(CHUNKS, RING, *tile),
            f32(2, PLANES, *tile), f32(CHUNKS, 5, PLANES, *tile), f32(5, DEPTH, WIDTH, WIDTH), f32(80, *tile),
            dma(5), dma(PHASES), dma(PHASES), dma(2 * CHUNKS),
        ],
        compiler_params=pltpu.CompilerParams(
            collective_id=0, has_side_effects=True, vmem_limit_bytes=16 * 1024 * 1024
        ),
    )(start_guess, forcing, initial, step_size, table, lamxy)


def solution(mesh):
    placed = (
        P("space", None, None),
        P("tm", "space", None, None),
        P("tm", None, "space", None, None),
        P("tm"),
    )
    return jax.shard_map(
        body,
        mesh=mesh,
        in_specs=placed,
        out_specs=P("tm", None, "space", None, None),
        check_vma=False,
    )
```

```python
import functools
import math

import jax
import jax.numpy as jnp
import numpy as np
from jax import lax
from jax.experimental import pallas as pl
from jax.experimental.pallas import tpu as pltpu
from jax.sharding import PartitionSpec as P

MESH = pl.DeviceIdType.MESH
GROUPS = 4
RING = 8
PLANES = 8
SPACES = 4
OWNERS = 2 * SPACES
DEPTH = PLANES // SPACES
WIDTH = 128
COLS = WIDTH // OWNERS
SUB = 8
SPLIT = SUB // 2
CHUNKS = COLS // SPLIT

OWNER_ORDER = (4, 3, 5, 2, 6, 1, 7)
RING_ORDER = (4, 3, 5, 2, 6, 1, 7)
GROUP_ORDER = (2, 1, 3)

FIRST, PSTEP, STEPS, GAINS, NEXT, SHIFT, GUESS = range(7)
FIELDS, SCAN, TOTALS, BACK, OUT = (8 + n * CHUNKS for n in range(5))
PHASES = 8 + 5 * CHUNKS


def node_tables():
    radical = math.sqrt(3.0 / 7.0)
    times = [0.0, (1.0 - radical) / 2.0, 0.5, (1.0 + radical) / 2.0, 1.0]
    integrals = np.zeros((4, 5))
    for column in range(5):
        coeffs = np.array([1.0])
        for other in range(5):
            if other != column:
                coeffs = np.convolve(coeffs, [-times[other], 1.0]) / (times[column] - times[other])
        powers = np.arange(1, 6)
        for section in range(4):
            integrals[section, column] = np.sum(
                coeffs * (times[section + 1] ** powers - times[section] ** powers) / powers
            )
    coarse = [0.0, 0.5, 1.0]
    interp = np.zeros((5, 3))
    for column in range(3):
        for section in range(5):
            weight = 1.0
            for other in range(3):
                if other != column:
                    weight *= (times[section] - coarse[other]) / (coarse[column] - coarse[other])
            interp[section, column] = weight
    return times, integrals, interp


TIMES, QUAD, INTERP = node_tables()
SPACING = [TIMES[m + 1] - TIMES[m] for m in range(4)]


def mixed(weights, values):
    total = None
    for weight, value in zip(weights, values):
        if value is None or abs(weight) < 1e-14:
            continue
        term = float(weight) * value
        total = term if total is None else total + term
    return total


def sweep(u, q, mu):
    v = [u[0]]
    for m in range(4):
        weights = list(QUAD[m])
        weights[m] -= SPACING[m]
        rate = mixed(weights + [SPACING[m]], u + [v[m]])
        new = -mu * rate
        if q is not None:
            new = new + q[m]
        if v[m] is not None:
            new = new + v[m]
        v.append(new)
    return v


def coarse_terms(v, q, mu):
    weights = QUAD[0] + QUAD[1]
    weights[0] -= 0.5
    left = -mu * mixed(weights, v)
    weights = QUAD[2] + QUAD[3]
    weights[2] -= 0.5
    right = -mu * mixed(weights, v)
    if q is not None:
        left = left + (q[0] + q[1])
        right = right + (q[2] + q[3])
    return left, right


def sources(q, guess, before, mu):
    rho = 1.0 - 0.5 * mu
    v = sweep([before, guess, guess, guess, guess], q, mu)
    left, right = coarse_terms(v, q, mu)
    forced = rho * left + right
    u = [None, None, left, None, forced]
    for m in (1, 3):
        u[m] = v[m] + mixed(INTERP[m], [-before, left - v[2], forced - v[4]])
    v = sweep(u, q, mu)
    left2, right2 = coarse_terms(v, q, mu)
    return forced, v, left2, rho * left2 + right2


def responses(mu):
    rho = 1.0 - 0.5 * mu
    square = rho * rho
    u = [1.0, None, rho, None, square]
    for m in (1, 3):
        u[m] = float(INTERP[m, 0]) + float(INTERP[m, 1]) * rho + float(INTERP[m, 2]) * square
    v = sweep(u, None, mu)
    left, right = coarse_terms(v, None, mu)
    return rho, square, v, left, rho * left + right


def sine(length):
    k = np.arange(1, length + 1)
    return math.sqrt(2.0 / (length + 1)) * np.sin(math.pi / (length + 1) * np.outer(k, k))


def eigen(length):
    return 2.0 - 2.0 * np.cos(math.pi / (length + 1) * np.arange(1, length + 1))


def along_z(planes, matrix):
    n = len(planes)
    half = n // 2
    even = [planes[i] + planes[n - 1 - i] for i in range(half)]
    odd = [planes[i] - planes[n - 1 - i] for i in range(half)]
    out = []
    for k in range(n):
        out.append(mixed(matrix[k][:half], even if k % 2 == 0 else odd))
    return out


def kernel(
    start_hbm, force_hbm, first_hbm, step_ref, sin_hbm, lamxy_hbm, out_ref,
    f_raw, g_raw, i_raw, sin_ref, lamxy, sin_hi, sin_lo, hat, gin, qin, firsts, early, ghat, shifted, guess,
    earlier, qhat, lam, tab, alpha, pair_steps, step_tile, all_steps, gains, gain_all, fb, scan_in,
    totals, partial, back, cd, starts, yout, outr, measure, load_sem, send_sem, recv_sem, local_sem,
):
    tm = lax.axis_index("tm")
    sp = lax.axis_index("space")
    pair, half = tm // 2, tm % 2
    group, slot = pair // RING, pair % RING
    own = half * SPACES + sp

    def halves(x):
        hi = x.astype(jnp.bfloat16)
        return hi, (x - hi.astype(jnp.float32)).astype(jnp.bfloat16)

    def product(a, b):
        dot = functools.partial(jnp.dot, preferred_element_type=jnp.float32)
        return dot(a[0], b[0]) + (dot(a[0], b[1]) + dot(a[1], b[0]))

    def matrix():
        return sin_hi[...], sin_lo[...]

    def owner(d):
        other = lax.rem(own + d, OWNERS)
        return other, (pair * 2 + other // SPACES, lax.rem(other, SPACES))

    def along_ring(d):
        other = lax.rem(slot + d, RING)
        return other, ((group * RING + other) * 2 + half, sp)

    def across(d):
        return ((lax.rem(group + d, GROUPS) * RING + slot) * 2 + half, sp)

    sent = {}

    def describe(src, dst, leaving, phase, target):
        return pltpu.make_async_remote_copy(
            src_ref=src, dst_ref=dst, send_sem=send_sem.at[leaving], recv_sem=recv_sem.at[phase],
            device_id=target, device_id_type=MESH,
        )

    def send(src, dst, phase, target):
        describe(src, dst, 0, phase, target).start()
        sent[phase] = sent.get(phase, 0) + math.prod(src.shape)

    def settle(sem, count):
        some = measure.at[pl.ds(0, count // (SUB * WIDTH))]
        pltpu.make_async_copy(some, some, sem).wait()

    def arrived(phase):
        settle(recv_sem.at[phase], sent[phase])

    pairs = GROUPS * RING
    following = (lax.rem(pair + 1, pairs) * 2 + half, sp)
    preceding = (lax.rem(pair + pairs - 1, pairs) * 2 + half, sp)
    partner = (pair * 2 + 1 - half, lax.rem(sp + SPACES // 2, SPACES))

    loads = [
        pltpu.make_async_copy(start_hbm.at[0], g_raw, load_sem.at[0]),
        pltpu.make_async_copy(sin_hbm, sin_ref, load_sem.at[1]),
        pltpu.make_async_copy(first_hbm, i_raw, load_sem.at[4]),
        pltpu.make_async_copy(force_hbm.at[0], f_raw, load_sem.at[2]),
        pltpu.make_async_copy(lamxy_hbm.at[pl.ds(pl.multiple_of(own * COLS, COLS), COLS)], lamxy, load_sem.at[3]),
    ]
    for load in loads:
        load.start()

    barrier = pltpu.get_barrier_semaphore()

    def greet(target):
        pl.semaphore_signal(barrier, inc=1, device_id=target, device_id_type=MESH)

    for d in RING_ORDER:
        greet(along_ring(d)[1])
    for d in range(SPACES):
        greet((lax.rem(pair + pairs - 1, pairs) * 2 + 1, lax.rem(sp + d, SPACES)))
    greet(following)
    greet(preceding)
    for d in GROUP_ORDER:
        greet(across(d))
    for d in OWNER_ORDER:
        greet(owner(d)[1])

    for load in loads[:3]:
        load.wait()
    step = step_ref[0]
    pair_steps[half] = jnp.full((SUB, WIDTH), step, jnp.float32)
    sin_hi[...], sin_lo[...] = halves(sin_ref[...])

    def transform(first, planes):
        count = len(planes)
        wide = product(matrix(), halves(jnp.concatenate(planes, axis=1)))
        tall = jnp.concatenate([wide[:, z * WIDTH : (z + 1) * WIDTH] for z in range(count)], axis=0)
        tall = product(halves(tall), matrix()).reshape(count // DEPTH, DEPTH, WIDTH, WIDTH)
        hat[pl.ds(first, count // DEPTH)] = tall

    transform(4, [g_raw[z] for z in range(DEPTH)] + [i_raw[z] for z in range(DEPTH)])
    loads[3].wait()

    def transform_fields(some):
        transform(some[0], [
            step * mixed(QUAD[m], [f_raw[j, z] for j in range(5)]) for m in some for z in range(DEPTH)
        ])

    transform_fields((0,))
    pl.semaphore_wait(barrier, OWNERS + RING + GROUPS - 1 + OWNERS * half)

    mine = pl.ds(pl.multiple_of(own * COLS, COLS), COLS)
    here = pl.ds(sp * DEPTH, DEPTH)
    part = pl.ds(pl.multiple_of(half * SPLIT, SPLIT), SPLIT)

    def slab(other, first, size):
        return pl.ds(pl.multiple_of(other * COLS + first, SPLIT), size)

    def swap(x):
        return pltpu.roll(x, SPLIT, x.ndim - 2)

    def pick(upper, lower):
        row = lax.broadcasted_iota(jnp.int32, (SUB, WIDTH), 0)
        return jnp.where(row < SPLIT, upper, lower)

    next_pair = lax.rem(pair + 1, pairs)

    @pl.when(half == 1)
    def _():
        for d in OWNER_ORDER + (0,):
            other = lax.rem(own + d, OWNERS)
            describe(
                hat.at[4, :, slab(other, 0, SUB), :], early.at[here], 1, NEXT,
                (next_pair * 2 + other // SPACES, lax.rem(other, SPACES)),
            ).start()

    send(pair_steps.at[half], pair_steps.at[half], PSTEP, partner)
    def send_guess(n):
        for d in OWNER_ORDER:
            other, target = owner(d)
            rows = pl.ds(n * SUB, SUB)
            send(hat.at[4, :, slab(other, n * SUB, SUB), :], gin.at[half, here, rows, :], GUESS + n, target)

    send_guess(0)
    first_size = (SPACES - 1) * DEPTH * COLS * WIDTH

    @pl.when(pair == 0)
    def _():
        for d in range(1, SPACES):
            other = lax.rem(sp + d, SPACES)
            describe(
                hat.at[5, :, slab(half * SPACES + other, 0, COLS), :], firsts.at[here], 2, FIRST, (tm, other)
            ).start()
        firsts[here] = hat[5, :, mine, :]

    transform_fields((1, 2, 3))
    gin[half, here] = hat[4, :, mine, :]

    def send_fields(h):
        for d in OWNER_ORDER:
            other, target = owner(d)
            send(
                hat.at[pl.ds(0, 4), :, slab(other, h * SPLIT, SPLIT), :], qin.at[h, :, here, part, :],
                FIELDS + h, target,
            )

    send_fields(0)
    send_guess(1)
    for h in range(1, CHUNKS):
        send_fields(h)
    kept = [
        pltpu.make_async_copy(
            hat.at[pl.ds(0, 4), :, slab(own, h * SPLIT, SPLIT), :], qin.at[h, :, here, part, :], local_sem.at[h]
        )
        for h in range(CHUNKS)
    ]
    for copy in kept:
        copy.start()

    loads[4].wait()

    z_matrix = sine(PLANES)
    z_eigen = eigen(PLANES)
    for h in range(CHUNKS):
        both = lamxy[pl.ds(h // 2 * SUB, SUB), :]
        both = pick(both, swap(both)) if h % 2 == 0 else pick(swap(both), both)
        for k in range(PLANES):
            lam[h, k] = both + float(z_eigen[k])

    def take_guess(n):
        arrived(GUESS + n)
        for s in (1, 0):
            planes = along_z([gin[s, z, pl.ds(n * SUB, SUB), :] for z in range(PLANES)], z_matrix)
            for k in range(PLANES):
                ghat[s, n, k] = planes[k]
            if s == 1 and n == 1:
                send(ghat.at[1, n], shifted.at[n], SHIFT, following)
        for h in (2 * n, 2 * n + 1):
            for k in range(PLANES):
                upper, lower = ghat[0, n, k], ghat[1, n, k]
                guess[h, k] = pick(upper, swap(lower)) if h % 2 == 0 else pick(swap(upper), lower)

    take_guess(0)
    arrived(PSTEP)
    step_tile[...] = pick(pair_steps[0], pair_steps[1])
    for d in RING_ORDER:
        send(step_tile, all_steps.at[slot], STEPS, along_ring(d)[1])
    all_steps[slot] = step_tile[...]
    def table(i, carry):
        two = pl.ds(i * 2, 2)
        for h in range(CHUNKS):
            mu = step_tile[...] * lam[h, two]
            rho, square, v, left, a = responses(mu)
            tab[h, 0, two] = left
            tab[h, 1, two] = rho
            tab[h, 2, two] = a
            tab[h, 3, two] = square
            for n, m in enumerate((1, 3)):
                w = [float(x) for x in INTERP[m]]
                tab[h, 4 + 2 * n, two] = v[m] - w[0] + w[1] * (left - v[2]) + w[2] * (a - v[4])
                tab[h, 5 + 2 * n, two] = w[0] + w[1] * rho + w[2] * square
            tab[h, 8, two] = pick(1.0, swap(square))
            tab[h, 9, two] = pick(0.0, swap(a))
        return carry

    lax.fori_loop(0, PLANES // 2, table, 0)

    opening = pick(jnp.where(pair == 0, 1.0, 0.0), 0.0)

    def pre(h):
        def step_pre(i, carry):
            two = pl.ds(i * 4, 4)
            mu = step_tile[...] * lam[h, two]
            before = earlier[h, two]
            f, v, left, b = sources([qhat[m, two] for m in range(4)], guess[h, two], before, mu)
            alpha[h, 0, two] = left
            alpha[h, 1, two] = b
            for n, m in enumerate((1, 3)):
                w = [float(x) for x in INTERP[m]]
                alpha[h, 2 + n, two] = v[m] + w[1] * (left - v[2]) + w[2] * (b - v[4])
            alpha[h, 4, two] = pick(0.0, swap(f))
            alpha[h, 5, two] = pick(0.0, swap(b))
            begin = before * opening
            square, a = tab[h, 3, two], tab[h, 2, two]
            f = f + square * begin
            b = b + (square + a) * begin
            first_f, first_b = swap(f), swap(b)
            pair_f = square * first_f + f
            pair_b = square * first_b + (a * first_f + b)
            fb[h, two] = pick(swap(pair_f), pair_b)
            return carry

        lax.fori_loop(0, PLANES // 4, step_pre, 0)

    zero = jnp.zeros((SUB, WIDTH), jnp.float32)

    def gain():
        arrived(STEPS)

        def pair_gain(i, carry):
            out = []
            for h in range(CHUNKS):
                total_g, total_a = carry[h]
                gains[i, 2, h] = total_g
                gains[i, 3, h] = total_a
                _, square, _, _, a = responses(all_steps[i] * lam[h, slot])
                other = swap(square)
                g = square * other
                a = other * a
                a = a + swap(a)
                gains[i, 0, h] = g
                gains[i, 1, h] = a
                out.append((g * total_g, g * total_a + a * total_g))
            return tuple(out)

        ones = jnp.ones((SUB, WIDTH), jnp.float32)
        ends = lax.fori_loop(0, RING, pair_gain, ((ones, zero),) * CHUNKS, unroll=4)
        for h in range(CHUNKS):
            gain_all[group, 0, h] = ends[h][0]
            gain_all[group, 1, h] = ends[h][1]
        for d in GROUP_ORDER:
            send(gain_all.at[group], gain_all.at[group], GAINS, across(d))

    for h in range(CHUNKS):
        if h == CHUNKS - 1:
            gain()
        kept[h].wait()
        arrived(FIELDS + h)
        for m in range(4):
            planes = along_z([qin[h, m, z] for z in range(PLANES)], z_matrix)
            for k in range(PLANES):
                qhat[m, k] = planes[k]
        if h % 2 == 0:
            n = h // 2
            if n == 0:
                settle(recv_sem.at[NEXT], PLANES * SUB * WIDTH)
                planes = along_z([early[z] for z in range(PLANES)], z_matrix)
                for k in range(PLANES):
                    shifted[n, k] = planes[k]
            else:
                arrived(SHIFT)

            @pl.when(pair == 0)
            def _():
                if h == 0:
                    settle(recv_sem.at[FIRST], first_size)
                planes = along_z([firsts[z, pl.ds(n * SUB, SUB), :] for z in range(PLANES)], z_matrix)
                for k in range(PLANES):
                    shifted[n, k] = planes[k]

            for k in range(PLANES):
                upper, lower = shifted[n, k], ghat[0, n, k]
                earlier[h, k] = pick(upper, swap(lower))
                earlier[h + 1, k] = pick(swap(upper), lower)
        pre(h)
        for d in RING_ORDER:
            other, target = along_ring(d)
            send(fb.at[h, other], scan_in.at[h, slot], SCAN + h, target)
        scan_in[h, slot] = fb[h, slot]
        if h == 0:
            take_guess(1)

    def advance(h):
        arrived(SCAN + h)
        c, d = zero, zero
        for i in range(RING):
            f = scan_in[h, i]
            b = swap(f)
            partial[h, i, 0] = c
            partial[h, i, 1] = d
            g, a = gains[i, 0, h], gains[i, 1, h]
            c, d = g * c + f, g * d + (a * c + b)
        totals[h, group] = pick(c, swap(d))
        for n in GROUP_ORDER:
            send(totals.at[h, group], totals.at[h, group], TOTALS + h, across(n))

    def fold(h):
        if h == 0:
            arrived(GAINS)
        arrived(TOTALS + h)
        c, d = zero, zero
        start_c, start_d = zero, zero
        for other in range(GROUPS - 1):
            g, a = gain_all[other, 0, h], gain_all[other, 1, h]
            f = totals[h, other]
            c, d = g * c + f, g * d + (a * c + swap(f))
            start_c = jnp.where(group == other + 1, c, start_c)
            start_d = jnp.where(group == other + 1, d, start_d)
        for i in range(RING):
            g, a = gains[i, 2, h], gains[i, 3, h]
            c = partial[h, i, 0] + g * start_c
            d = partial[h, i, 1] + (g * start_d + a * start_c)
            back[h, i] = pick(c, swap(d))
        for n in RING_ORDER:
            other, target = along_ring(n)
            send(back.at[h, other], cd.at[h, slot], BACK + h, target)
        cd[h, slot] = back[h, slot]

    returned = []

    def give(h):
        arrived(BACK + h)

        @pl.when(pair == 0)
        def _():
            for k in range(PLANES):
                before = earlier[h, k]
                cd[h, k] = pick(before, swap(before))

        for k in range(PLANES):
            tile = cd[h, k]
            turned = swap(tile)
            c, d = pick(tile, turned), pick(turned, tile)
            starts[0, k] = tab[h, 8, k] * c + alpha[h, 4, k]
            starts[1, k] = tab[h, 8, k] * d + (tab[h, 9, k] * c + alpha[h, 5, k])
        rows = []
        for m in range(5):
            planes = []
            for k in range(PLANES):
                if m == 0:
                    planes.append(starts[1, k])
                else:
                    n = {2: 0, 4: 1, 1: 2, 3: 3}[m]
                    planes.append(
                        alpha[h, n, k] + (tab[h, 2 * n, k] * starts[0, k] + tab[h, 2 * n + 1, k] * starts[1, k])
                    )
            rows += along_z(planes, z_matrix)
        rows = product(halves(jnp.concatenate(rows, axis=0)), matrix())
        yout[h] = rows.reshape(5, PLANES, SUB, WIDTH)
        for d in OWNER_ORDER:
            other, target = owner(d)
            rows = pl.ds(pl.multiple_of(other // SPACES * SPLIT, SPLIT), SPLIT)
            send(
                yout.at[h, :, pl.ds(lax.rem(other, SPACES) * DEPTH, DEPTH), rows, :],
                outr.at[:, :, slab(own, h * SPLIT, SPLIT), :], OUT + h, target,
            )
        copy = pltpu.make_async_copy(
            yout.at[h, :, here, part, :], outr.at[:, :, slab(own, h * SPLIT, SPLIT), :], local_sem.at[CHUNKS + h]
        )
        copy.start()
        returned.append(copy)

    for h in range(CHUNKS - 1):
        advance(h)
    fold(0)
    advance(CHUNKS - 1)
    for h in range(1, CHUNKS):
        fold(h)
    for h in range(CHUNKS):
        give(h)

    for h in range(CHUNKS):
        returned[h].wait()
        arrived(OUT + h)
    for m in range(5):
        wide = jnp.concatenate([outr[m, z] for z in range(DEPTH)], axis=1)
        wide = product(matrix(), halves(wide))
        for z in range(DEPTH):
            out_ref[0, m, z] = wide[:, z * WIDTH : (z + 1) * WIDTH]

    settle(send_sem.at[0], sum(sent.values()))

    @pl.when(half == 1)
    def _():
        settle(send_sem.at[1], OWNERS * DEPTH * SUB * WIDTH)

    @pl.when(pair == 0)
    def _():
        settle(send_sem.at[2], first_size)


def body(initial, start_guess, forcing, step_size):
    table = jnp.asarray(sine(WIDTH), jnp.float32)
    lamxy = jnp.asarray(eigen(WIDTH)[:, None] + eigen(WIDTH)[None, :], jnp.float32)
    hbm = pl.BlockSpec(memory_space=pltpu.HBM)
    f32 = lambda *shape: pltpu.VMEM(shape, jnp.float32)
    dma = lambda *shape: pltpu.SemaphoreType.DMA(shape)
    tile = (SUB, WIDTH)
    bf16 = pltpu.VMEM((WIDTH, WIDTH), jnp.bfloat16)
    start_guess, forcing, initial, table, lamxy = (
        pltpu.with_memory_space_constraint(x, pltpu.HBM)
        for x in (start_guess, forcing, initial, table, lamxy)
    )
    return pl.pallas_call(
        kernel,
        out_shape=jax.ShapeDtypeStruct((1, 5, DEPTH, WIDTH, WIDTH), jnp.float32),
        in_specs=[hbm, hbm, hbm, pl.BlockSpec(memory_space=pltpu.SMEM), hbm, hbm],
        out_specs=pl.BlockSpec(memory_space=pltpu.VMEM),
        scratch_shapes=[
            f32(5, DEPTH, WIDTH, WIDTH), f32(DEPTH, WIDTH, WIDTH), f32(DEPTH, WIDTH, WIDTH),
            f32(WIDTH, WIDTH), f32(COLS, WIDTH), bf16, bf16, f32(6, DEPTH, WIDTH, WIDTH),
            f32(2, PLANES, COLS, WIDTH), f32(CHUNKS, 4, PLANES, *tile), f32(PLANES, COLS, WIDTH), f32(PLANES, *tile),
            f32(2, COLS // SUB, PLANES, *tile), f32(COLS // SUB, PLANES, *tile), f32(CHUNKS, PLANES, *tile),
            f32(CHUNKS, PLANES, *tile), f32(4, PLANES, *tile), f32(CHUNKS, PLANES, *tile),
            f32(CHUNKS, 10, PLANES, *tile), f32(CHUNKS, 6, PLANES, *tile), f32(2, *tile), f32(*tile),
            f32(RING, *tile), f32(RING, 4, CHUNKS, *tile), f32(GROUPS, 2, CHUNKS, *tile),
            f32(CHUNKS, RING, *tile), f32(CHUNKS, RING, *tile), f32(CHUNKS, GROUPS, *tile),
            f32(CHUNKS, RING, 2, *tile), f32(CHUNKS, RING, *tile), f32(CHUNKS, RING, *tile),
            f32(2, PLANES, *tile), f32(CHUNKS, 5, PLANES, *tile), f32(5, DEPTH, WIDTH, WIDTH), f32(480, *tile),
            dma(5), dma(3), dma(PHASES), dma(2 * CHUNKS),
        ],
        compiler_params=pltpu.CompilerParams(
            collective_id=0, has_side_effects=True, vmem_limit_bytes=16 * 1024 * 1024
        ),
    )(start_guess, forcing, initial, step_size, table, lamxy)


def solution(mesh):
    placed = (
        P("space", None, None),
        P("tm", "space", None, None),
        P("tm", None, "space", None, None),
        P("tm"),
    )
    return jax.shard_map(
        body,
        mesh=mesh,
        in_specs=placed,
        out_specs=P("tm", None, "space", None, None),
        check_vma=False,
    )
```

```python
import functools
import math

import jax
import jax.numpy as jnp
import numpy as np
from jax import lax
from jax.experimental import pallas as pl
from jax.experimental.pallas import tpu as pltpu
from jax.sharding import PartitionSpec as P

MESH = pl.DeviceIdType.MESH
GROUPS = 4
RING = 8
PLANES = 8
SPACES = 4
OWNERS = 2 * SPACES
DEPTH = PLANES // SPACES
WIDTH = 128
COLS = WIDTH // OWNERS
SUB = 8
SPLIT = SUB // 2
CHUNKS = COLS // SPLIT

OWNER_ORDER = (4, 3, 5, 2, 6, 1, 7)
RING_ORDER = (4, 3, 5, 2, 6, 1, 7)
GROUP_ORDER = (2, 1, 3)

FIRST, PSTEP, STEPS, GAINS, NEXT, SHIFT, GUESS = range(7)
FIELDS, SCAN, TOTALS, BACK, OUT = (8 + n * CHUNKS for n in range(5))
PHASES = 8 + 5 * CHUNKS


def node_tables():
    radical = math.sqrt(3.0 / 7.0)
    times = [0.0, (1.0 - radical) / 2.0, 0.5, (1.0 + radical) / 2.0, 1.0]
    integrals = np.zeros((4, 5))
    for column in range(5):
        coeffs = np.array([1.0])
        for other in range(5):
            if other != column:
                coeffs = np.convolve(coeffs, [-times[other], 1.0]) / (times[column] - times[other])
        powers = np.arange(1, 6)
        for section in range(4):
            integrals[section, column] = np.sum(
                coeffs * (times[section + 1] ** powers - times[section] ** powers) / powers
            )
    coarse = [0.0, 0.5, 1.0]
    interp = np.zeros((5, 3))
    for column in range(3):
        for section in range(5):
            weight = 1.0
            for other in range(3):
                if other != column:
                    weight *= (times[section] - coarse[other]) / (coarse[column] - coarse[other])
            interp[section, column] = weight
    return times, integrals, interp


TIMES, QUAD, INTERP = node_tables()
SPACING = [TIMES[m + 1] - TIMES[m] for m in range(4)]


def mixed(weights, values):
    total = None
    for weight, value in zip(weights, values):
        if value is None or abs(weight) < 1e-14:
            continue
        term = float(weight) * value
        total = term if total is None else total + term
    return total


def sweep(u, q, mu):
    v = [u[0]]
    for m in range(4):
        weights = list(QUAD[m])
        weights[m] -= SPACING[m]
        rate = mixed(weights + [SPACING[m]], u + [v[m]])
        new = -mu * rate
        if q is not None:
            new = new + q[m]
        if v[m] is not None:
            new = new + v[m]
        v.append(new)
    return v


def coarse_terms(v, q, mu):
    weights = QUAD[0] + QUAD[1]
    weights[0] -= 0.5
    left = -mu * mixed(weights, v)
    weights = QUAD[2] + QUAD[3]
    weights[2] -= 0.5
    right = -mu * mixed(weights, v)
    if q is not None:
        left = left + (q[0] + q[1])
        right = right + (q[2] + q[3])
    return left, right


def sources(q, guess, before, mu):
    rho = 1.0 - 0.5 * mu
    v = sweep([before, guess, guess, guess, guess], q, mu)
    left, right = coarse_terms(v, q, mu)
    forced = rho * left + right
    u = [None, None, left, None, forced]
    for m in (1, 3):
        u[m] = v[m] + mixed(INTERP[m], [-before, left - v[2], forced - v[4]])
    v = sweep(u, q, mu)
    left2, right2 = coarse_terms(v, q, mu)
    return forced, v, left2, rho * left2 + right2


def responses(mu):
    rho = 1.0 - 0.5 * mu
    square = rho * rho
    u = [1.0, None, rho, None, square]
    for m in (1, 3):
        u[m] = float(INTERP[m, 0]) + float(INTERP[m, 1]) * rho + float(INTERP[m, 2]) * square
    v = sweep(u, None, mu)
    left, right = coarse_terms(v, None, mu)
    return rho, square, v, left, rho * left + right


def sine(length):
    k = np.arange(1, length + 1)
    return math.sqrt(2.0 / (length + 1)) * np.sin(math.pi / (length + 1) * np.outer(k, k))


def eigen(length):
    return 2.0 - 2.0 * np.cos(math.pi / (length + 1) * np.arange(1, length + 1))


def along_z(planes, matrix):
    n = len(planes)
    half = n // 2
    even = [planes[i] + planes[n - 1 - i] for i in range(half)]
    odd = [planes[i] - planes[n - 1 - i] for i in range(half)]
    out = []
    for k in range(n):
        out.append(mixed(matrix[k][:half], even if k % 2 == 0 else odd))
    return out


def kernel(
    start_hbm, force_hbm, first_hbm, step_ref, sin_hbm, lamxy_hbm, out_ref,
    f_raw, g_raw, i_raw, sin_ref, lamxy, sin_left, sin_right, hat, gin, qin, firsts, early, ghat, shifted, guess,
    earlier, qhat, lam, tab, alpha, pair_steps, step_tile, all_steps, gains, gain_all, fb, scan_in,
    totals, partial, back, cd, starts, yout, outr, measure, load_sem, send_sem, recv_sem, local_sem,
):
    tm = lax.axis_index("tm")
    sp = lax.axis_index("space")
    pair, half = tm // 2, tm % 2
    group, slot = pair // RING, pair % RING
    own = half * SPACES + sp

    def halves(x):
        hi = x.astype(jnp.bfloat16)
        return hi, (x - hi.astype(jnp.float32)).astype(jnp.bfloat16)

    def from_left(x):
        hi, lo = halves(x)
        return jnp.dot(sin_left[...], jnp.concatenate([hi, lo, hi], axis=0), preferred_element_type=jnp.float32)

    def from_right(x):
        hi, lo = halves(x)
        return jnp.dot(jnp.concatenate([hi, hi, lo], axis=1), sin_right[...], preferred_element_type=jnp.float32)

    def owner(d):
        other = lax.rem(own + d, OWNERS)
        return other, (pair * 2 + other // SPACES, lax.rem(other, SPACES))

    def along_ring(d):
        other = lax.rem(slot + d, RING)
        return other, ((group * RING + other) * 2 + half, sp)

    def across(d):
        return ((lax.rem(group + d, GROUPS) * RING + slot) * 2 + half, sp)

    sent = {}

    def describe(src, dst, leaving, phase, target):
        return pltpu.make_async_remote_copy(
            src_ref=src, dst_ref=dst, send_sem=send_sem.at[leaving], recv_sem=recv_sem.at[phase],
            device_id=target, device_id_type=MESH,
        )

    def send(src, dst, phase, target):
        describe(src, dst, 0, phase, target).start()
        sent[phase] = sent.get(phase, 0) + math.prod(src.shape)

    def settle(sem, count):
        some = measure.at[pl.ds(0, count // (SUB * WIDTH))]
        pltpu.make_async_copy(some, some, sem).wait()

    def arrived(phase):
        settle(recv_sem.at[phase], sent[phase])

    pairs = GROUPS * RING
    following = (lax.rem(pair + 1, pairs) * 2 + half, sp)
    preceding = (lax.rem(pair + pairs - 1, pairs) * 2 + half, sp)
    partner = (pair * 2 + 1 - half, lax.rem(sp + SPACES // 2, SPACES))

    loads = [
        pltpu.make_async_copy(start_hbm.at[0], g_raw, load_sem.at[0]),
        pltpu.make_async_copy(sin_hbm, sin_ref, load_sem.at[1]),
        pltpu.make_async_copy(first_hbm, i_raw, load_sem.at[4]),
        pltpu.make_async_copy(force_hbm.at[0], f_raw, load_sem.at[2]),
        pltpu.make_async_copy(lamxy_hbm.at[pl.ds(pl.multiple_of(own * COLS, COLS), COLS)], lamxy, load_sem.at[3]),
    ]
    for load in loads:
        load.start()

    barrier = pltpu.get_barrier_semaphore()

    def greet(target):
        pl.semaphore_signal(barrier, inc=1, device_id=target, device_id_type=MESH)

    for d in RING_ORDER:
        greet(along_ring(d)[1])
    for d in range(SPACES):
        greet((lax.rem(pair + pairs - 1, pairs) * 2 + 1, lax.rem(sp + d, SPACES)))
    greet(following)
    greet(preceding)
    for d in GROUP_ORDER:
        greet(across(d))
    for d in OWNER_ORDER:
        greet(owner(d)[1])

    for load in loads[:3]:
        load.wait()
    step = step_ref[0]
    pair_steps[half] = jnp.full((SUB, WIDTH), step, jnp.float32)
    hi, lo = halves(sin_ref[...])
    sin_left[...] = jnp.concatenate([hi, hi, lo], axis=1)
    sin_right[...] = jnp.concatenate([hi, lo, hi], axis=0)

    def transform(first, planes):
        count = len(planes)
        wide = from_left(jnp.concatenate(planes, axis=1))
        tall = jnp.concatenate([wide[:, z * WIDTH : (z + 1) * WIDTH] for z in range(count)], axis=0)
        tall = from_right(tall).reshape(count // DEPTH, DEPTH, WIDTH, WIDTH)
        hat[pl.ds(first, count // DEPTH)] = tall

    transform(4, [g_raw[z] for z in range(DEPTH)] + [i_raw[z] for z in range(DEPTH)])
    loads[3].wait()

    def transform_fields(some):
        transform(some[0], [
            step * mixed(QUAD[m], [f_raw[j, z] for j in range(5)]) for m in some for z in range(DEPTH)
        ])

    transform_fields((0,))
    pl.semaphore_wait(barrier, OWNERS + RING + GROUPS - 1 + OWNERS * half)

    mine = pl.ds(pl.multiple_of(own * COLS, COLS), COLS)
    here = pl.ds(sp * DEPTH, DEPTH)
    part = pl.ds(pl.multiple_of(half * SPLIT, SPLIT), SPLIT)

    def slab(other, first, size):
        return pl.ds(pl.multiple_of(other * COLS + first, SPLIT), size)

    def swap(x):
        return pltpu.roll(x, SPLIT, x.ndim - 2)

    def pick(upper, lower):
        row = lax.broadcasted_iota(jnp.int32, (SUB, WIDTH), 0)
        return jnp.where(row < SPLIT, upper, lower)

    next_pair = lax.rem(pair + 1, pairs)

    @pl.when(half == 1)
    def _():
        for d in OWNER_ORDER + (0,):
            other = lax.rem(own + d, OWNERS)
            describe(
                hat.at[4, :, slab(other, 0, SUB), :], early.at[here], 1, NEXT,
                (next_pair * 2 + other // SPACES, lax.rem(other, SPACES)),
            ).start()

    send(pair_steps.at[half], pair_steps.at[half], PSTEP, partner)
    def send_guess(n):
        for d in OWNER_ORDER:
            other, target = owner(d)
            rows = pl.ds(n * SUB, SUB)
            send(hat.at[4, :, slab(other, n * SUB, SUB), :], gin.at[half, here, rows, :], GUESS + n, target)

    send_guess(0)
    first_size = (SPACES - 1) * DEPTH * COLS * WIDTH

    @pl.when(pair == 0)
    def _():
        for d in range(1, SPACES):
            other = lax.rem(sp + d, SPACES)
            describe(
                hat.at[5, :, slab(half * SPACES + other, 0, COLS), :], firsts.at[here], 2, FIRST, (tm, other)
            ).start()
        firsts[here] = hat[5, :, mine, :]

    transform_fields((1, 2, 3))
    gin[half, here] = hat[4, :, mine, :]

    def send_fields(h):
        for d in OWNER_ORDER:
            other, target = owner(d)
            send(
                hat.at[pl.ds(0, 4), :, slab(other, h * SPLIT, SPLIT), :], qin.at[h, :, here, part, :],
                FIELDS + h, target,
            )

    send_fields(0)
    send_guess(1)
    for h in range(1, CHUNKS):
        send_fields(h)
    kept = [
        pltpu.make_async_copy(
            hat.at[pl.ds(0, 4), :, slab(own, h * SPLIT, SPLIT), :], qin.at[h, :, here, part, :], local_sem.at[h]
        )
        for h in range(CHUNKS)
    ]
    for copy in kept:
        copy.start()

    loads[4].wait()

    z_matrix = sine(PLANES)
    z_eigen = eigen(PLANES)
    for h in range(CHUNKS):
        both = lamxy[pl.ds(h // 2 * SUB, SUB), :]
        both = pick(both, swap(both)) if h % 2 == 0 else pick(swap(both), both)
        for k in range(PLANES):
            lam[h, k] = both + float(z_eigen[k])

    def take_guess(n):
        arrived(GUESS + n)
        for s in (1, 0):
            planes = along_z([gin[s, z, pl.ds(n * SUB, SUB), :] for z in range(PLANES)], z_matrix)
            for k in range(PLANES):
                ghat[s, n, k] = planes[k]
            if s == 1 and n == 1:
                send(ghat.at[1, n], shifted.at[n], SHIFT, following)
        for h in (2 * n, 2 * n + 1):
            for k in range(PLANES):
                upper, lower = ghat[0, n, k], ghat[1, n, k]
                guess[h, k] = pick(upper, swap(lower)) if h % 2 == 0 else pick(swap(upper), lower)

    take_guess(0)
    arrived(PSTEP)
    step_tile[...] = pick(pair_steps[0], pair_steps[1])
    for d in RING_ORDER:
        send(step_tile, all_steps.at[slot], STEPS, along_ring(d)[1])
    all_steps[slot] = step_tile[...]
    def table(i, carry):
        two = pl.ds(i * 2, 2)
        for h in range(CHUNKS):
            mu = step_tile[...] * lam[h, two]
            rho, square, v, left, a = responses(mu)
            tab[h, 0, two] = left
            tab[h, 1, two] = rho
            tab[h, 2, two] = a
            tab[h, 3, two] = square
            for n, m in enumerate((1, 3)):
                w = [float(x) for x in INTERP[m]]
                tab[h, 4 + 2 * n, two] = v[m] - w[0] + w[1] * (left - v[2]) + w[2] * (a - v[4])
                tab[h, 5 + 2 * n, two] = w[0] + w[1] * rho + w[2] * square
            tab[h, 8, two] = pick(1.0, swap(square))
            tab[h, 9, two] = pick(0.0, swap(a))
        return carry

    lax.fori_loop(0, PLANES // 2, table, 0)

    opening = pick(jnp.where(pair == 0, 1.0, 0.0), 0.0)

    def pre(h):
        def step_pre(i, carry):
            two = pl.ds(i * 4, 4)
            mu = step_tile[...] * lam[h, two]
            before = earlier[h, two]
            f, v, left, b = sources([qhat[m, two] for m in range(4)], guess[h, two], before, mu)
            alpha[h, 0, two] = left
            alpha[h, 1, two] = b
            for n, m in enumerate((1, 3)):
                w = [float(x) for x in INTERP[m]]
                alpha[h, 2 + n, two] = v[m] + w[1] * (left - v[2]) + w[2] * (b - v[4])
            alpha[h, 4, two] = pick(0.0, swap(f))
            alpha[h, 5, two] = pick(0.0, swap(b))
            begin = before * opening
            square, a = tab[h, 3, two], tab[h, 2, two]
            f = f + square * begin
            b = b + (square + a) * begin
            first_f, first_b = swap(f), swap(b)
            pair_f = square * first_f + f
            pair_b = square * first_b + (a * first_f + b)
            fb[h, two] = pick(swap(pair_f), pair_b)
            return carry

        lax.fori_loop(0, PLANES // 4, step_pre, 0)

    zero = jnp.zeros((SUB, WIDTH), jnp.float32)

    def gain():
        arrived(STEPS)

        def pair_gain(i, carry):
            out = []
            for h in range(CHUNKS):
                total_g, total_a = carry[h]
                gains[i, 2, h] = total_g
                gains[i, 3, h] = total_a
                _, square, _, _, a = responses(all_steps[i] * lam[h, slot])
                other = swap(square)
                g = square * other
                a = other * a
                a = a + swap(a)
                gains[i, 0, h] = g
                gains[i, 1, h] = a
                out.append((g * total_g, g * total_a + a * total_g))
            return tuple(out)

        ones = jnp.ones((SUB, WIDTH), jnp.float32)
        ends = lax.fori_loop(0, RING, pair_gain, ((ones, zero),) * CHUNKS, unroll=4)
        for h in range(CHUNKS):
            gain_all[group, 0, h] = ends[h][0]
            gain_all[group, 1, h] = ends[h][1]
        for d in GROUP_ORDER:
            send(gain_all.at[group], gain_all.at[group], GAINS, across(d))

    for h in range(CHUNKS):
        if h == CHUNKS - 1:
            gain()
        kept[h].wait()
        arrived(FIELDS + h)
        for m in range(4):
            planes = along_z([qin[h, m, z] for z in range(PLANES)], z_matrix)
            for k in range(PLANES):
                qhat[m, k] = planes[k]
        if h % 2 == 0:
            n = h // 2
            if n == 0:
                settle(recv_sem.at[NEXT], PLANES * SUB * WIDTH)
                planes = along_z([early[z] for z in range(PLANES)], z_matrix)
                for k in range(PLANES):
                    shifted[n, k] = planes[k]
            else:
                arrived(SHIFT)

            @pl.when(pair == 0)
            def _():
                if h == 0:
                    settle(recv_sem.at[FIRST], first_size)
                planes = along_z([firsts[z, pl.ds(n * SUB, SUB), :] for z in range(PLANES)], z_matrix)
                for k in range(PLANES):
                    shifted[n, k] = planes[k]

            for k in range(PLANES):
                upper, lower = shifted[n, k], ghat[0, n, k]
                earlier[h, k] = pick(upper, swap(lower))
                earlier[h + 1, k] = pick(swap(upper), lower)
        pre(h)
        for d in RING_ORDER:
            other, target = along_ring(d)
            send(fb.at[h, other], scan_in.at[h, slot], SCAN + h, target)
        scan_in[h, slot] = fb[h, slot]
        if h == 0:
            take_guess(1)

    def advance(h):
        arrived(SCAN + h)
        c, d = zero, zero
        for i in range(RING):
            f = scan_in[h, i]
            b = swap(f)
            partial[h, i, 0] = c
            partial[h, i, 1] = d
            g, a = gains[i, 0, h], gains[i, 1, h]
            c, d = g * c + f, g * d + (a * c + b)
        totals[h, group] = pick(c, swap(d))
        for n in GROUP_ORDER:
            send(totals.at[h, group], totals.at[h, group], TOTALS + h, across(n))

    def fold(h):
        if h == 0:
            arrived(GAINS)
        arrived(TOTALS + h)
        c, d = zero, zero
        start_c, start_d = zero, zero
        for other in range(GROUPS - 1):
            g, a = gain_all[other, 0, h], gain_all[other, 1, h]
            f = totals[h, other]
            c, d = g * c + f, g * d + (a * c + swap(f))
            start_c = jnp.where(group == other + 1, c, start_c)
            start_d = jnp.where(group == other + 1, d, start_d)
        for i in range(RING):
            g, a = gains[i, 2, h], gains[i, 3, h]
            c = partial[h, i, 0] + g * start_c
            d = partial[h, i, 1] + (g * start_d + a * start_c)
            back[h, i] = pick(c, swap(d))
        for n in RING_ORDER:
            other, target = along_ring(n)
            send(back.at[h, other], cd.at[h, slot], BACK + h, target)
        cd[h, slot] = back[h, slot]

    returned = []

    def give(h):
        arrived(BACK + h)

        @pl.when(pair == 0)
        def _():
            for k in range(PLANES):
                before = earlier[h, k]
                cd[h, k] = pick(before, swap(before))

        for k in range(PLANES):
            tile = cd[h, k]
            turned = swap(tile)
            c, d = pick(tile, turned), pick(turned, tile)
            starts[0, k] = tab[h, 8, k] * c + alpha[h, 4, k]
            starts[1, k] = tab[h, 8, k] * d + (tab[h, 9, k] * c + alpha[h, 5, k])
        rows = []
        for m in range(5):
            planes = []
            for k in range(PLANES):
                if m == 0:
                    planes.append(starts[1, k])
                else:
                    n = {2: 0, 4: 1, 1: 2, 3: 3}[m]
                    planes.append(
                        alpha[h, n, k] + (tab[h, 2 * n, k] * starts[0, k] + tab[h, 2 * n + 1, k] * starts[1, k])
                    )
            rows += along_z(planes, z_matrix)
        rows = from_right(jnp.concatenate(rows, axis=0))
        yout[h] = rows.reshape(5, PLANES, SUB, WIDTH)
        for d in OWNER_ORDER:
            other, target = owner(d)
            rows = pl.ds(pl.multiple_of(other // SPACES * SPLIT, SPLIT), SPLIT)
            send(
                yout.at[h, :, pl.ds(lax.rem(other, SPACES) * DEPTH, DEPTH), rows, :],
                outr.at[:, :, slab(own, h * SPLIT, SPLIT), :], OUT + h, target,
            )
        copy = pltpu.make_async_copy(
            yout.at[h, :, here, part, :], outr.at[:, :, slab(own, h * SPLIT, SPLIT), :], local_sem.at[CHUNKS + h]
        )
        copy.start()
        returned.append(copy)

    for h in range(CHUNKS - 1):
        advance(h)
    fold(0)
    advance(CHUNKS - 1)
    for h in range(1, CHUNKS):
        fold(h)
    for h in range(CHUNKS):
        give(h)

    for h in range(CHUNKS):
        returned[h].wait()
        arrived(OUT + h)
    for m in range(5):
        wide = jnp.concatenate([outr[m, z] for z in range(DEPTH)], axis=1)
        wide = from_left(wide)
        for z in range(DEPTH):
            out_ref[0, m, z] = wide[:, z * WIDTH : (z + 1) * WIDTH]

    settle(send_sem.at[0], sum(sent.values()))

    @pl.when(half == 1)
    def _():
        settle(send_sem.at[1], OWNERS * DEPTH * SUB * WIDTH)

    @pl.when(pair == 0)
    def _():
        settle(send_sem.at[2], first_size)


def body(initial, start_guess, forcing, step_size):
    table = jnp.asarray(sine(WIDTH), jnp.float32)
    lamxy = jnp.asarray(eigen(WIDTH)[:, None] + eigen(WIDTH)[None, :], jnp.float32)
    hbm = pl.BlockSpec(memory_space=pltpu.HBM)
    f32 = lambda *shape: pltpu.VMEM(shape, jnp.float32)
    dma = lambda *shape: pltpu.SemaphoreType.DMA(shape)
    tile = (SUB, WIDTH)
    start_guess, forcing, initial, table, lamxy = (
        pltpu.with_memory_space_constraint(x, pltpu.HBM)
        for x in (start_guess, forcing, initial, table, lamxy)
    )
    return pl.pallas_call(
        kernel,
        out_shape=jax.ShapeDtypeStruct((1, 5, DEPTH, WIDTH, WIDTH), jnp.float32),
        in_specs=[hbm, hbm, hbm, pl.BlockSpec(memory_space=pltpu.SMEM), hbm, hbm],
        out_specs=pl.BlockSpec(memory_space=pltpu.VMEM),
        scratch_shapes=[
            f32(5, DEPTH, WIDTH, WIDTH), f32(DEPTH, WIDTH, WIDTH), f32(DEPTH, WIDTH, WIDTH),
            f32(WIDTH, WIDTH), f32(COLS, WIDTH), pltpu.VMEM((WIDTH, 3 * WIDTH), jnp.bfloat16), pltpu.VMEM((3 * WIDTH, WIDTH), jnp.bfloat16), f32(6, DEPTH, WIDTH, WIDTH),
            f32(2, PLANES, COLS, WIDTH), f32(CHUNKS, 4, PLANES, *tile), f32(PLANES, COLS, WIDTH), f32(PLANES, *tile),
            f32(2, COLS // SUB, PLANES, *tile), f32(COLS // SUB, PLANES, *tile), f32(CHUNKS, PLANES, *tile),
            f32(CHUNKS, PLANES, *tile), f32(4, PLANES, *tile), f32(CHUNKS, PLANES, *tile),
            f32(CHUNKS, 10, PLANES, *tile), f32(CHUNKS, 6, PLANES, *tile), f32(2, *tile), f32(*tile),
            f32(RING, *tile), f32(RING, 4, CHUNKS, *tile), f32(GROUPS, 2, CHUNKS, *tile),
            f32(CHUNKS, RING, *tile), f32(CHUNKS, RING, *tile), f32(CHUNKS, GROUPS, *tile),
            f32(CHUNKS, RING, 2, *tile), f32(CHUNKS, RING, *tile), f32(CHUNKS, RING, *tile),
            f32(2, PLANES, *tile), f32(CHUNKS, 5, PLANES, *tile), f32(5, DEPTH, WIDTH, WIDTH), f32(480, *tile),
            dma(5), dma(3), dma(PHASES), dma(2 * CHUNKS),
        ],
        compiler_params=pltpu.CompilerParams(
            collective_id=0, has_side_effects=True, vmem_limit_bytes=16 * 1024 * 1024
        ),
    )(start_guess, forcing, initial, step_size, table, lamxy)


def solution(mesh):
    placed = (
        P("space", None, None),
        P("tm", "space", None, None),
        P("tm", None, "space", None, None),
        P("tm"),
    )
    return jax.shard_map(
        body,
        mesh=mesh,
        in_specs=placed,
        out_specs=P("tm", None, "space", None, None),
        check_vma=False,
    )
```

```python
import functools
import math

import jax
import jax.numpy as jnp
import numpy as np
from jax import lax
from jax.experimental import pallas as pl
from jax.experimental.pallas import tpu as pltpu
from jax.sharding import PartitionSpec as P

MESH = pl.DeviceIdType.MESH
GROUPS = 4
RING = 8
PLANES = 8
SPACES = 4
OWNERS = 2 * SPACES
DEPTH = PLANES // SPACES
WIDTH = 128
COLS = WIDTH // OWNERS
SUB = 8
SPLIT = SUB // 2
CHUNKS = COLS // SPLIT

OWNER_ORDER = (4, 3, 5, 2, 6, 1, 7)
RING_ORDER = (4, 3, 5, 2, 6, 1, 7)
GROUP_ORDER = (2, 1, 3)

FIRST, PSTEP, STEPS, GAINS, NEXT, SHIFT, GUESS = range(7)
FIELDS, SCAN, TOTALS, BACK, OUT = (8 + n * CHUNKS for n in range(5))
PHASES = 8 + 5 * CHUNKS


def node_tables():
    radical = math.sqrt(3.0 / 7.0)
    times = [0.0, (1.0 - radical) / 2.0, 0.5, (1.0 + radical) / 2.0, 1.0]
    integrals = np.zeros((4, 5))
    for column in range(5):
        coeffs = np.array([1.0])
        for other in range(5):
            if other != column:
                coeffs = np.convolve(coeffs, [-times[other], 1.0]) / (times[column] - times[other])
        powers = np.arange(1, 6)
        for section in range(4):
            integrals[section, column] = np.sum(
                coeffs * (times[section + 1] ** powers - times[section] ** powers) / powers
            )
    coarse = [0.0, 0.5, 1.0]
    interp = np.zeros((5, 3))
    for column in range(3):
        for section in range(5):
            weight = 1.0
            for other in range(3):
                if other != column:
                    weight *= (times[section] - coarse[other]) / (coarse[column] - coarse[other])
            interp[section, column] = weight
    return times, integrals, interp


TIMES, QUAD, INTERP = node_tables()
SPACING = [TIMES[m + 1] - TIMES[m] for m in range(4)]


def mixed(weights, values):
    total = None
    for weight, value in zip(weights, values):
        if value is None or abs(weight) < 1e-14:
            continue
        term = float(weight) * value
        total = term if total is None else total + term
    return total


def sweep(u, q, mu):
    v = [u[0]]
    for m in range(4):
        weights = list(QUAD[m])
        weights[m] -= SPACING[m]
        rate = mixed(weights + [SPACING[m]], u + [v[m]])
        new = -mu * rate
        if q is not None:
            new = new + q[m]
        if v[m] is not None:
            new = new + v[m]
        v.append(new)
    return v


def coarse_terms(v, q, mu):
    weights = QUAD[0] + QUAD[1]
    weights[0] -= 0.5
    left = -mu * mixed(weights, v)
    weights = QUAD[2] + QUAD[3]
    weights[2] -= 0.5
    right = -mu * mixed(weights, v)
    if q is not None:
        left = left + (q[0] + q[1])
        right = right + (q[2] + q[3])
    return left, right


def sources(q, guess, before, mu):
    rho = 1.0 - 0.5 * mu
    v = sweep([before, guess, guess, guess, guess], q, mu)
    left, right = coarse_terms(v, q, mu)
    forced = rho * left + right
    u = [None, None, left, None, forced]
    for m in (1, 3):
        u[m] = v[m] + mixed(INTERP[m], [-before, left - v[2], forced - v[4]])
    v = sweep(u, q, mu)
    left2, right2 = coarse_terms(v, q, mu)
    return forced, v, left2, rho * left2 + right2


def responses(mu):
    rho = 1.0 - 0.5 * mu
    square = rho * rho
    u = [1.0, None, rho, None, square]
    for m in (1, 3):
        u[m] = float(INTERP[m, 0]) + float(INTERP[m, 1]) * rho + float(INTERP[m, 2]) * square
    v = sweep(u, None, mu)
    left, right = coarse_terms(v, None, mu)
    return rho, square, v, left, rho * left + right


def sine(length):
    k = np.arange(1, length + 1)
    return math.sqrt(2.0 / (length + 1)) * np.sin(math.pi / (length + 1) * np.outer(k, k))


def eigen(length):
    return 2.0 - 2.0 * np.cos(math.pi / (length + 1) * np.arange(1, length + 1))


def along_z(planes, matrix):
    n = len(planes)
    half = n // 2
    even = [planes[i] + planes[n - 1 - i] for i in range(half)]
    odd = [planes[i] - planes[n - 1 - i] for i in range(half)]
    out = []
    for k in range(n):
        out.append(mixed(matrix[k][:half], even if k % 2 == 0 else odd))
    return out


def kernel(
    start_hbm, force_hbm, first_hbm, step_ref, sin_hbm, lamxy_hbm, out_ref,
    f_raw, g_raw, i_raw, sin_ref, lamxy, sin_left, sin_right, hat, gin, qin, firsts, early, ghat, shifted, guess,
    earlier, qhat, lam, tab, alpha, pair_steps, step_tile, all_steps, gains, gain_all, fb, scan_in,
    totals, partial, back, cd, starts, yout, outr, measure, load_sem, send_sem, recv_sem, local_sem,
):
    tm = lax.axis_index("tm")
    sp = lax.axis_index("space")
    pair, half = tm // 2, tm % 2
    group, slot = pair // RING, pair % RING
    own = half * SPACES + sp

    def halves(x):
        hi = x.astype(jnp.bfloat16)
        return hi, (x - hi.astype(jnp.float32)).astype(jnp.bfloat16)

    def from_left(x):
        hi, lo = halves(x)
        return jnp.dot(sin_left[...], jnp.concatenate([hi, lo, hi], axis=0), preferred_element_type=jnp.float32)

    def from_right(x):
        hi, lo = halves(x)
        return jnp.dot(jnp.concatenate([hi, hi, lo], axis=1), sin_right[...], preferred_element_type=jnp.float32)

    def owner(d):
        other = lax.rem(own + d, OWNERS)
        return other, (pair * 2 + other // SPACES, lax.rem(other, SPACES))

    def along_ring(d):
        other = lax.rem(slot + d, RING)
        return other, ((group * RING + other) * 2 + half, sp)

    def across(d):
        return ((lax.rem(group + d, GROUPS) * RING + slot) * 2 + half, sp)

    sent = {}

    def describe(src, dst, leaving, phase, target):
        return pltpu.make_async_remote_copy(
            src_ref=src, dst_ref=dst, send_sem=send_sem.at[leaving], recv_sem=recv_sem.at[phase],
            device_id=target, device_id_type=MESH,
        )

    def send(src, dst, phase, target):
        describe(src, dst, 0, phase, target).start()
        sent[phase] = sent.get(phase, 0) + math.prod(src.shape)

    def settle(sem, count):
        some = measure.at[pl.ds(0, count // (SUB * WIDTH))]
        pltpu.make_async_copy(some, some, sem).wait()

    def arrived(phase):
        settle(recv_sem.at[phase], sent[phase])

    pairs = GROUPS * RING
    following = (lax.rem(pair + 1, pairs) * 2 + half, sp)
    preceding = (lax.rem(pair + pairs - 1, pairs) * 2 + half, sp)
    partner = (pair * 2 + 1 - half, lax.rem(sp + SPACES // 2, SPACES))

    loads = [
        pltpu.make_async_copy(start_hbm.at[0], g_raw, load_sem.at[0]),
        pltpu.make_async_copy(sin_hbm, sin_ref, load_sem.at[1]),
        pltpu.make_async_copy(first_hbm, i_raw, load_sem.at[4]),
        pltpu.make_async_copy(force_hbm.at[0], f_raw, load_sem.at[2]),
        pltpu.make_async_copy(lamxy_hbm.at[pl.ds(pl.multiple_of(own * COLS, COLS), COLS)], lamxy, load_sem.at[3]),
    ]
    for load in loads:
        load.start()

    barrier = pltpu.get_barrier_semaphore()

    def greet(target):
        pl.semaphore_signal(barrier, inc=1, device_id=target, device_id_type=MESH)

    for d in RING_ORDER:
        greet(along_ring(d)[1])
    for d in range(SPACES):
        greet((lax.rem(pair + pairs - 1, pairs) * 2 + 1, lax.rem(sp + d, SPACES)))
    greet(following)
    greet(preceding)
    for d in GROUP_ORDER:
        greet(across(d))
    for d in OWNER_ORDER:
        greet(owner(d)[1])

    for load in loads[:3]:
        load.wait()
    step = step_ref[0]
    pair_steps[half] = jnp.full((SUB, WIDTH), step, jnp.float32)
    hi, lo = halves(sin_ref[...])
    sin_left[...] = jnp.concatenate([hi, hi, lo], axis=1)
    sin_right[...] = jnp.concatenate([hi, lo, hi], axis=0)

    def transform(first, planes):
        count = len(planes)
        wide = from_left(jnp.concatenate(planes, axis=1))
        tall = jnp.concatenate([wide[:, z * WIDTH : (z + 1) * WIDTH] for z in range(count)], axis=0)
        tall = from_right(tall).reshape(count // DEPTH, DEPTH, WIDTH, WIDTH)
        hat[pl.ds(first, count // DEPTH)] = tall

    transform(4, [g_raw[z] for z in range(DEPTH)] + [i_raw[z] for z in range(DEPTH)])
    loads[3].wait()

    def transform_fields(some):
        transform(some[0], [
            step * mixed(QUAD[m], [f_raw[j, z] for j in range(5)]) for m in some for z in range(DEPTH)
        ])

    transform_fields((0,))
    pl.semaphore_wait(barrier, OWNERS + RING + GROUPS - 1 + OWNERS * half)

    mine = pl.ds(pl.multiple_of(own * COLS, COLS), COLS)
    here = pl.ds(sp * DEPTH, DEPTH)
    part = pl.ds(pl.multiple_of(half * SPLIT, SPLIT), SPLIT)

    def slab(other, first, size):
        return pl.ds(pl.multiple_of(other * COLS + first, SPLIT), size)

    def swap(x):
        return pltpu.roll(x, SPLIT, x.ndim - 2)

    def pick(upper, lower):
        row = lax.broadcasted_iota(jnp.int32, (SUB, WIDTH), 0)
        return jnp.where(row < SPLIT, upper, lower)

    next_pair = lax.rem(pair + 1, pairs)

    @pl.when(half == 1)
    def _():
        for d in OWNER_ORDER + (0,):
            other = lax.rem(own + d, OWNERS)
            describe(
                hat.at[4, :, slab(other, 0, SUB), :], early.at[here], 1, NEXT,
                (next_pair * 2 + other // SPACES, lax.rem(other, SPACES)),
            ).start()

    send(pair_steps.at[half], pair_steps.at[half], PSTEP, partner)
    def send_guess(n):
        for d in OWNER_ORDER:
            other, target = owner(d)
            rows = pl.ds(n * SUB, SUB)
            send(hat.at[4, :, slab(other, n * SUB, SUB), :], gin.at[half, here, rows, :], GUESS + n, target)

    send_guess(0)
    send_guess(1)
    first_size = (SPACES - 1) * DEPTH * COLS * WIDTH

    @pl.when(pair == 0)
    def _():
        for d in range(1, SPACES):
            other = lax.rem(sp + d, SPACES)
            describe(
                hat.at[5, :, slab(half * SPACES + other, 0, COLS), :], firsts.at[here], 2, FIRST, (tm, other)
            ).start()
        firsts[here] = hat[5, :, mine, :]

    transform_fields((1, 2, 3))
    gin[half, here] = hat[4, :, mine, :]

    def send_fields(h):
        for d in OWNER_ORDER:
            other, target = owner(d)
            send(
                hat.at[pl.ds(0, 4), :, slab(other, h * SPLIT, SPLIT), :], qin.at[h, :, here, part, :],
                FIELDS + h, target,
            )

    send_fields(0)
    for h in range(1, CHUNKS):
        send_fields(h)
    kept = [
        pltpu.make_async_copy(
            hat.at[pl.ds(0, 4), :, slab(own, h * SPLIT, SPLIT), :], qin.at[h, :, here, part, :], local_sem.at[h]
        )
        for h in range(CHUNKS)
    ]
    for copy in kept:
        copy.start()

    loads[4].wait()

    z_matrix = sine(PLANES)
    z_eigen = eigen(PLANES)
    for h in range(CHUNKS):
        both = lamxy[pl.ds(h // 2 * SUB, SUB), :]
        both = pick(both, swap(both)) if h % 2 == 0 else pick(swap(both), both)
        for k in range(PLANES):
            lam[h, k] = both + float(z_eigen[k])

    def take_guess(n):
        arrived(GUESS + n)
        for s in (1, 0):
            planes = along_z([gin[s, z, pl.ds(n * SUB, SUB), :] for z in range(PLANES)], z_matrix)
            for k in range(PLANES):
                ghat[s, n, k] = planes[k]
            if s == 1 and n == 1:
                send(ghat.at[1, n], shifted.at[n], SHIFT, following)
        for h in (2 * n, 2 * n + 1):
            for k in range(PLANES):
                upper, lower = ghat[0, n, k], ghat[1, n, k]
                guess[h, k] = pick(upper, swap(lower)) if h % 2 == 0 else pick(swap(upper), lower)

    take_guess(0)
    arrived(PSTEP)
    step_tile[...] = pick(pair_steps[0], pair_steps[1])
    for d in RING_ORDER:
        send(step_tile, all_steps.at[slot], STEPS, along_ring(d)[1])
    all_steps[slot] = step_tile[...]
    def table(i, carry):
        two = pl.ds(i * 2, 2)
        for h in range(CHUNKS):
            mu = step_tile[...] * lam[h, two]
            rho, square, v, left, a = responses(mu)
            tab[h, 0, two] = left
            tab[h, 1, two] = rho
            tab[h, 2, two] = a
            tab[h, 3, two] = square
            for n, m in enumerate((1, 3)):
                w = [float(x) for x in INTERP[m]]
                tab[h, 4 + 2 * n, two] = v[m] - w[0] + w[1] * (left - v[2]) + w[2] * (a - v[4])
                tab[h, 5 + 2 * n, two] = w[0] + w[1] * rho + w[2] * square
            tab[h, 8, two] = pick(1.0, swap(square))
            tab[h, 9, two] = pick(0.0, swap(a))
        return carry

    lax.fori_loop(0, PLANES // 2, table, 0)

    take_guess(1)
    opening = pick(jnp.where(pair == 0, 1.0, 0.0), 0.0)

    def pre(h):
        def step_pre(i, carry):
            two = pl.ds(i * 8, 8)
            mu = step_tile[...] * lam[h, two]
            before = earlier[h, two]
            f, v, left, b = sources([qhat[m, two] for m in range(4)], guess[h, two], before, mu)
            alpha[h, 0, two] = left
            alpha[h, 1, two] = b
            for n, m in enumerate((1, 3)):
                w = [float(x) for x in INTERP[m]]
                alpha[h, 2 + n, two] = v[m] + w[1] * (left - v[2]) + w[2] * (b - v[4])
            alpha[h, 4, two] = pick(0.0, swap(f))
            alpha[h, 5, two] = pick(0.0, swap(b))
            begin = before * opening
            square, a = tab[h, 3, two], tab[h, 2, two]
            f = f + square * begin
            b = b + (square + a) * begin
            first_f, first_b = swap(f), swap(b)
            pair_f = square * first_f + f
            pair_b = square * first_b + (a * first_f + b)
            fb[h, two] = pick(swap(pair_f), pair_b)
            return carry

        lax.fori_loop(0, 1, step_pre, 0)

    zero = jnp.zeros((SUB, WIDTH), jnp.float32)

    def gain():
        arrived(STEPS)

        def pair_gain(i, carry):
            out = []
            for h in range(CHUNKS):
                total_g, total_a = carry[h]
                gains[i, 2, h] = total_g
                gains[i, 3, h] = total_a
                _, square, _, _, a = responses(all_steps[i] * lam[h, slot])
                other = swap(square)
                g = square * other
                a = other * a
                a = a + swap(a)
                gains[i, 0, h] = g
                gains[i, 1, h] = a
                out.append((g * total_g, g * total_a + a * total_g))
            return tuple(out)

        ones = jnp.ones((SUB, WIDTH), jnp.float32)
        ends = lax.fori_loop(0, RING, pair_gain, ((ones, zero),) * CHUNKS, unroll=8)
        for h in range(CHUNKS):
            gain_all[group, 0, h] = ends[h][0]
            gain_all[group, 1, h] = ends[h][1]
        for d in GROUP_ORDER:
            send(gain_all.at[group], gain_all.at[group], GAINS, across(d))

    for h in range(CHUNKS):
        if h == CHUNKS - 1:
            gain()
        kept[h].wait()
        arrived(FIELDS + h)
        for m in range(4):
            planes = along_z([qin[h, m, z] for z in range(PLANES)], z_matrix)
            for k in range(PLANES):
                qhat[m, k] = planes[k]
        if h % 2 == 0:
            n = h // 2
            if n == 0:
                settle(recv_sem.at[NEXT], PLANES * SUB * WIDTH)
                planes = along_z([early[z] for z in range(PLANES)], z_matrix)
                for k in range(PLANES):
                    shifted[n, k] = planes[k]
            else:
                arrived(SHIFT)

            @pl.when(pair == 0)
            def _():
                if h == 0:
                    settle(recv_sem.at[FIRST], first_size)
                planes = along_z([firsts[z, pl.ds(n * SUB, SUB), :] for z in range(PLANES)], z_matrix)
                for k in range(PLANES):
                    shifted[n, k] = planes[k]

            for k in range(PLANES):
                upper, lower = shifted[n, k], ghat[0, n, k]
                earlier[h, k] = pick(upper, swap(lower))
                earlier[h + 1, k] = pick(swap(upper), lower)
        pre(h)
        for d in RING_ORDER:
            other, target = along_ring(d)
            send(fb.at[h, other], scan_in.at[h, slot], SCAN + h, target)
        scan_in[h, slot] = fb[h, slot]

    def advance(h):
        arrived(SCAN + h)
        c, d = zero, zero
        for i in range(RING):
            f = scan_in[h, i]
            b = swap(f)
            partial[h, i, 0] = c
            partial[h, i, 1] = d
            g, a = gains[i, 0, h], gains[i, 1, h]
            c, d = g * c + f, g * d + (a * c + b)
        totals[h, group] = pick(c, swap(d))
        for n in GROUP_ORDER:
            send(totals.at[h, group], totals.at[h, group], TOTALS + h, across(n))

    def fold(h):
        if h == 0:
            arrived(GAINS)
        arrived(TOTALS + h)
        c, d = zero, zero
        start_c, start_d = zero, zero
        for other in range(GROUPS - 1):
            g, a = gain_all[other, 0, h], gain_all[other, 1, h]
            f = totals[h, other]
            c, d = g * c + f, g * d + (a * c + swap(f))
            start_c = jnp.where(group == other + 1, c, start_c)
            start_d = jnp.where(group == other + 1, d, start_d)
        for i in range(RING):
            g, a = gains[i, 2, h], gains[i, 3, h]
            c = partial[h, i, 0] + g * start_c
            d = partial[h, i, 1] + (g * start_d + a * start_c)
            back[h, i] = pick(c, swap(d))
        for n in RING_ORDER:
            other, target = along_ring(n)
            send(back.at[h, other], cd.at[h, slot], BACK + h, target)
        cd[h, slot] = back[h, slot]

    returned = []

    def give(h):
        arrived(BACK + h)

        @pl.when(pair == 0)
        def _():
            for k in range(PLANES):
                before = earlier[h, k]
                cd[h, k] = pick(before, swap(before))

        for k in range(PLANES):
            tile = cd[h, k]
            turned = swap(tile)
            c, d = pick(tile, turned), pick(turned, tile)
            starts[0, k] = tab[h, 8, k] * c + alpha[h, 4, k]
            starts[1, k] = tab[h, 8, k] * d + (tab[h, 9, k] * c + alpha[h, 5, k])
        rows = []
        for m in range(5):
            planes = []
            for k in range(PLANES):
                if m == 0:
                    planes.append(starts[1, k])
                else:
                    n = {2: 0, 4: 1, 1: 2, 3: 3}[m]
                    planes.append(
                        alpha[h, n, k] + (tab[h, 2 * n, k] * starts[0, k] + tab[h, 2 * n + 1, k] * starts[1, k])
                    )
            rows += along_z(planes, z_matrix)
        rows = from_right(jnp.concatenate(rows, axis=0))
        yout[h] = rows.reshape(5, PLANES, SUB, WIDTH)
        for d in OWNER_ORDER:
            other, target = owner(d)
            rows = pl.ds(pl.multiple_of(other // SPACES * SPLIT, SPLIT), SPLIT)
            send(
                yout.at[h, :, pl.ds(lax.rem(other, SPACES) * DEPTH, DEPTH), rows, :],
                outr.at[:, :, slab(own, h * SPLIT, SPLIT), :], OUT + h, target,
            )
        copy = pltpu.make_async_copy(
            yout.at[h, :, here, part, :], outr.at[:, :, slab(own, h * SPLIT, SPLIT), :], local_sem.at[CHUNKS + h]
        )
        copy.start()
        returned.append(copy)

    for h in range(CHUNKS - 1):
        advance(h)
    fold(0)
    advance(CHUNKS - 1)
    for h in range(1, CHUNKS):
        fold(h)
    for h in range(CHUNKS):
        give(h)

    for h in range(CHUNKS):
        returned[h].wait()
        arrived(OUT + h)
    for m in range(5):
        wide = jnp.concatenate([outr[m, z] for z in range(DEPTH)], axis=1)
        wide = from_left(wide)
        for z in range(DEPTH):
            out_ref[0, m, z] = wide[:, z * WIDTH : (z + 1) * WIDTH]

    settle(send_sem.at[0], sum(sent.values()))

    @pl.when(half == 1)
    def _():
        settle(send_sem.at[1], OWNERS * DEPTH * SUB * WIDTH)

    @pl.when(pair == 0)
    def _():
        settle(send_sem.at[2], first_size)


def body(initial, start_guess, forcing, step_size):
    table = jnp.asarray(sine(WIDTH), jnp.float32)
    lamxy = jnp.asarray(eigen(WIDTH)[:, None] + eigen(WIDTH)[None, :], jnp.float32)
    hbm = pl.BlockSpec(memory_space=pltpu.HBM)
    f32 = lambda *shape: pltpu.VMEM(shape, jnp.float32)
    dma = lambda *shape: pltpu.SemaphoreType.DMA(shape)
    tile = (SUB, WIDTH)
    start_guess, forcing, initial, table, lamxy = (
        pltpu.with_memory_space_constraint(x, pltpu.HBM)
        for x in (start_guess, forcing, initial, table, lamxy)
    )
    return pl.pallas_call(
        kernel,
        out_shape=jax.ShapeDtypeStruct((1, 5, DEPTH, WIDTH, WIDTH), jnp.float32),
        in_specs=[hbm, hbm, hbm, pl.BlockSpec(memory_space=pltpu.SMEM), hbm, hbm],
        out_specs=pl.BlockSpec(memory_space=pltpu.VMEM),
        scratch_shapes=[
            f32(5, DEPTH, WIDTH, WIDTH), f32(DEPTH, WIDTH, WIDTH), f32(DEPTH, WIDTH, WIDTH),
            f32(WIDTH, WIDTH), f32(COLS, WIDTH), pltpu.VMEM((WIDTH, 3 * WIDTH), jnp.bfloat16), pltpu.VMEM((3 * WIDTH, WIDTH), jnp.bfloat16), f32(6, DEPTH, WIDTH, WIDTH),
            f32(2, PLANES, COLS, WIDTH), f32(CHUNKS, 4, PLANES, *tile), f32(PLANES, COLS, WIDTH), f32(PLANES, *tile),
            f32(2, COLS // SUB, PLANES, *tile), f32(COLS // SUB, PLANES, *tile), f32(CHUNKS, PLANES, *tile),
            f32(CHUNKS, PLANES, *tile), f32(4, PLANES, *tile), f32(CHUNKS, PLANES, *tile),
            f32(CHUNKS, 10, PLANES, *tile), f32(CHUNKS, 6, PLANES, *tile), f32(2, *tile), f32(*tile),
            f32(RING, *tile), f32(RING, 4, CHUNKS, *tile), f32(GROUPS, 2, CHUNKS, *tile),
            f32(CHUNKS, RING, *tile), f32(CHUNKS, RING, *tile), f32(CHUNKS, GROUPS, *tile),
            f32(CHUNKS, RING, 2, *tile), f32(CHUNKS, RING, *tile), f32(CHUNKS, RING, *tile),
            f32(2, PLANES, *tile), f32(CHUNKS, 5, PLANES, *tile), f32(5, DEPTH, WIDTH, WIDTH), f32(480, *tile),
            dma(5), dma(3), dma(PHASES), dma(2 * CHUNKS),
        ],
        compiler_params=pltpu.CompilerParams(
            collective_id=0, has_side_effects=True, vmem_limit_bytes=16 * 1024 * 1024
        ),
    )(start_guess, forcing, initial, step_size, table, lamxy)


def solution(mesh):
    placed = (
        P("space", None, None),
        P("tm", "space", None, None),
        P("tm", None, "space", None, None),
        P("tm"),
    )
    return jax.shard_map(
        body,
        mesh=mesh,
        in_specs=placed,
        out_specs=P("tm", None, "space", None, None),
        check_vma=False,
    )
```
